32 devices in a mesh: local: 4 (over z), data: 8 (over y, x, core).
Axes of the slice: x: 2, y: 2, z: 4, core: 2. Of those that a mesh axis runs over, the one named last changes fastest.
Arguments:
- tokens: bfloat16 [32768, 1280], P(('data', 'local'))
- cotangent: bfloat16 [32768, 1280], P(('data', 'local'))
- w_up: bfloat16 [3, 1280, 5120], P(None, ('data', 'local'))
- w_down: bfloat16 [3, 5120, 1280], P(None, ('data', 'local'))
- lora_a: float32 [3, 1280, 4], replicated
- lora_b: float32 [3, 4, 5120], replicated
Outputs:
- output 1: bfloat16 [32768, 1280], P(('data', 'local'))
- output 2: bfloat16 [32768, 1280], P(('data', 'local'))
- output 3: float32 [3, 1280, 4], replicated
- output 4: float32 [3, 4, 5120], replicated
All inputs are finite; a program needn't handle non-finite values.
Results may differ from the reference program's by a relative error of at most 0.0163844.
Values are sent between devices in bfloat16 or wider.
A program may use at most 1 GiB of HBM per device.

```python
import jax
import jax.numpy as jnp
from jax import lax

TOKENS = 1024
NUM_DEVICES = 32
HIDDEN = 1280
FF_DIM = 5120
RANK = 4
LAYERS = 3

TOTAL_TOKENS = NUM_DEVICES * TOKENS


def setup_inputs(seed: int = 0) -> dict:
    keys = jax.random.split(jax.random.key(seed), 6)
    tokens = jax.random.normal(keys[0], (TOTAL_TOKENS, HIDDEN), jnp.float32).astype(jnp.bfloat16)
    cotangent = jax.random.normal(keys[1], (TOTAL_TOKENS, HIDDEN), jnp.float32).astype(jnp.bfloat16)
    w_up = (jax.random.normal(keys[2], (LAYERS, HIDDEN, FF_DIM), jnp.float32) * HIDDEN ** -0.5).astype(jnp.bfloat16)
    w_down = (jax.random.normal(keys[3], (LAYERS, FF_DIM, HIDDEN), jnp.float32) * FF_DIM ** -0.5).astype(jnp.bfloat16)
    lora_a = jax.random.normal(keys[4], (LAYERS, HIDDEN, RANK), jnp.float32) * HIDDEN ** -0.5
    lora_b = jax.random.normal(keys[5], (LAYERS, RANK, FF_DIM), jnp.float32) * (0.5 / RANK) ** 0.5
    return {"tokens": tokens, "cotangent": cotangent, "w_up": w_up, "w_down": w_down, "lora_a": lora_a, "lora_b": lora_b}


def layer_forward(resid, w_in, w_out, adapt_a, adapt_b):
    resid_f = resid.astype(jnp.float32)
    inv_rms = lax.rsqrt(jnp.mean(resid_f * resid_f, axis=-1, keepdims=True) + 1e-6)
    normed = (resid_f * inv_rms).astype(jnp.bfloat16)
    low_rank = jnp.dot(normed.astype(jnp.float32), adapt_a)
    pre_act = (jnp.dot(normed, w_in, preferred_element_type=jnp.float32) + jnp.dot(low_rank, adapt_b)).astype(jnp.bfloat16)
    hidden_act = jax.nn.gelu(pre_act.astype(jnp.float32), approximate=True).astype(jnp.bfloat16)
    return (resid_f + jnp.dot(hidden_act, w_out, preferred_element_type=jnp.float32)).astype(jnp.bfloat16)


def stack_forward(resid, w_up, w_down, lora_a, lora_b):
    def body(carry, weights):
        w_in, w_out, adapt_a, adapt_b = weights
        return layer_forward(carry, w_in, w_out, adapt_a, adapt_b), None
    result, _ = lax.scan(body, resid, (w_up, w_down, lora_a, lora_b))
    return result


def reference(tokens, cotangent, w_up, w_down, lora_a, lora_b):
    tok_blocks = tokens.reshape(NUM_DEVICES, TOKENS, HIDDEN)
    cot_blocks = cotangent.reshape(NUM_DEVICES, TOKENS, HIDDEN)

    def block_step(running, pair):
        blk_tokens, blk_cot = pair
        result, pullback = jax.vjp(lambda blk_in, adapt_a, adapt_b: stack_forward(blk_in, w_up, w_down, adapt_a, adapt_b), blk_tokens, lora_a, lora_b)
        grad_x, grad_a, grad_b = pullback(blk_cot)
        return (running[0] + grad_a, running[1] + grad_b), (result, grad_x)

    start_sums = (jnp.zeros(lora_a.shape, jnp.float32), jnp.zeros(lora_b.shape, jnp.float32))
    (sum_a, sum_b), (out_blocks, grad_blocks) = lax.scan(block_step, start_sums, (tok_blocks, cot_blocks))
    return (out_blocks.reshape(TOTAL_TOKENS, HIDDEN), grad_blocks.reshape(TOTAL_TOKENS, HIDDEN), sum_a, sum_b)
```

```python
import math

import jax
import jax.numpy as jnp
from jax import lax
from jax.experimental import pallas as pl
from jax.experimental.pallas import tpu as pltpu
from jax.sharding import PartitionSpec as P

GROUP = ("data", "local")
MESH = pl.DeviceIdType.MESH
BF16, F32 = jnp.bfloat16, jnp.float32
ROWS = 512
LANES = 128
NORM_EPS = 1e-6
GELU_S = math.sqrt(2.0 / math.pi)
GELU_C = 0.044715

LAYERS, TOKENS, HIDDEN, FF, RANK = 3, 1024, 1280, 5120, 4
NT = 10
TILES = 2 * LAYERS * NT
UP_ROWS, DOWN_ROWS = HIDDEN // 32, FF // 32
UP_TILE, DOWN_TILE = FF // NT, DOWN_ROWS // NT
OUT_COLS = 256
QUARTER = FF // 4
RING, SRING = 20, 16
OFFSETS = (7, 6, 5, 4, 3, 2, 1, 0, -1)
LEAD = OFFSETS[0]
FUSED_FROM = 5 * NT
SUB = 256
SUBS = QUARTER // SUB
G_COLS = 3328
G_HALF = G_COLS // 2
G_EDGE = (FF + HIDDEN) // 2
G_STAGES = 6
SPLITS = (((0, 424), (424, 424), (848, 432)), ((0, 88), (88, 88), (176, 80)))


def dot(a, b):
    return jnp.dot(a, b, preferred_element_type=F32)


def dot_t(a, b):
    return lax.dot_general(a, b, (((1,), (1,)), ((), ())), preferred_element_type=F32)


def split3(x):
    hi = x.astype(BF16).astype(F32)
    rest = x - hi
    mid = rest.astype(BF16).astype(F32)
    return hi, mid, (rest - mid).astype(BF16).astype(F32)


def stack_left(x):
    hi, mid, lo = split3(x)
    return hi, hi, hi, mid, mid, lo


def stack_right(x):
    hi, mid, lo = split3(x)
    return hi, mid, lo, hi, mid, hi


def sum3(x):
    return x[0:8] + x[8:16] + x[16:24]


def gelu_inner(x):
    x2 = x * x
    return x2, jnp.tanh(x * (GELU_S + (GELU_S * GELU_C) * x2))


def step_kernel(
    tokens, cotangent, w_up, w_down, adapt_a, adapt_b,
    out_tokens, grad_tokens, grad_a, grad_b,
    land_up, land_down, back_up, back_down, pre_acts, resids, normeds,
    own_up, own_down, x, u, d, inv_s, b6, a6, v6, v3, dlow, gb, send_g, half_g, recv_first, recv_half, recv_last,
    recv_sem, pair_sem, send_sem, back_recv, back_send, swap_recv, swap_send, g_recv, g_send, load_sem, back_sem, w_sem, act_sem, keep_sem, credit,
):
    z = lax.axis_index("local")
    dev = lax.axis_index("data")
    core = lax.rem(dev, 2)
    dx = dev + 2 - 4 * lax.rem(dev // 2, 2)
    dy = dev + 4 - 8 * (dev // 4)
    dd = dx + dy - dev
    dc = dev + 1 - 2 * core
    zp = z + 1 - 2 * lax.rem(z, 2)
    za, zb = 3 - z, 3 - zp
    parity = lax.rem(lax.rem(dev // 2, 2) + dev // 4 + z, 2)
    is_end = jnp.logical_or(z == 0, z == 3)
    is_mid = jnp.logical_not(is_end)
    to_p, to_a, to_b = (zp, dev), (za, dev), (zb, dev)
    to_x, to_y, to_c = (z, dx), (z, dy), (z, dc)
    cols = (dev, dx, dy, dd)
    pair_cols = (dc, dc + dx - dev, dc + dy - dev, dc + dd - dev)

    def remote(src, dst, ssem, rsem, target):
        return pltpu.make_async_remote_copy(src, dst, ssem, rsem, device_id=target, device_id_type=MESH)

    def both(cond, on, off):
        pl.when(cond)(on)
        pl.when(jnp.logical_not(cond))(off)

    loads = [
        pltpu.make_async_copy(w_up, own_up, load_sem.at[0]),
        pltpu.make_async_copy(w_down, own_down, load_sem.at[1]),
        pltpu.make_async_copy(tokens, x, load_sem.at[2]),
        pltpu.make_async_copy(cotangent, d, load_sem.at[3]),
    ]
    for load in loads:
        load.start()
    barrier = pltpu.get_barrier_semaphore()
    for target in (to_p, to_x, to_y, to_c, to_b):
        pl.semaphore_signal(barrier, inc=1, device_id=target, device_id_type=MESH)

    @pl.when(is_mid)
    def _():
        pl.semaphore_signal(barrier, inc=1, device_id=to_a, device_id_type=MESH)
        pl.semaphore_wait(barrier, 6)

    @pl.when(is_end)
    def _():
        pl.semaphore_wait(barrier, 5)

    loads[0].wait()
    loads[1].wait()

    def is_up(k):
        m = k // NT
        return jnp.logical_or(jnp.logical_and(lax.rem(m, 2) == 0, m < 4), m == 5)

    def slab(up, k, col, zz, own=False):
        layer, t, n = k // (2 * NT), lax.rem(k, NT), 4 * col + zz
        slot = lax.rem(layer, 2)
        if up:
            c = pl.ds(pl.multiple_of(UP_TILE * t, LANES), UP_TILE)
            return own_up.at[layer, :, c] if own else land_up.at[slot, pl.ds(pl.multiple_of(UP_ROWS * n, 8), UP_ROWS), c]
        r = pl.multiple_of(DOWN_TILE * t, 16)
        return own_down.at[layer, pl.ds(r, DOWN_TILE), :] if own else land_down.at[slot, pl.ds(pl.multiple_of(DOWN_ROWS * n + r, 16), DOWN_TILE), :]

    def send(up, k, entry):
        rel, zz, target, to_rel = entry
        own = rel == own_c and zz is z
        index = [e is entry for e in order].index(True)
        return remote(slab(up, k, cols[rel], zz, own), slab(up, k, cols[rel], zz), send_sem.at[lax.rem(k, SRING), index],
                      recv_sem.at[lax.rem(k, RING), to_rel * 4 + zz], target)

    def wait_slab(up, k, rel, zz):
        s = slab(up, k, cols[rel], zz)
        remote(s, s, send_sem.at[0, 0], recv_sem.at[lax.rem(k, RING), rel * 4 + zz], to_x).wait_recv()

    def pair_copy(up, k, g, c):
        layer, t = k // (2 * NT), lax.rem(k, NT)
        slot = lax.rem(layer, 2)
        if up:
            s = land_up.at[slot, pl.ds(pl.multiple_of(4 * UP_ROWS * c, 8), 4 * UP_ROWS), pl.ds(pl.multiple_of(UP_TILE * t, LANES), UP_TILE)]
        else:
            s = land_down.reshape(2, 32, DOWN_ROWS, HIDDEN).at[slot, pl.ds(4 * c, 4), pl.ds(pl.multiple_of(DOWN_TILE * t, 16), DOWN_TILE), :]
        return remote(s, s, send_sem.at[lax.rem(k, SRING), len(order) + 1 + g], pair_sem.at[lax.rem(k, RING), g], to_c)

    own_c, x_c, y_c, diag_c = range(4)
    own_sends = [(own_c, z, to_p, own_c), (own_c, z, to_a, own_c), (own_c, z, to_x, x_c), (own_c, z, to_y, y_c)]
    hop_p = [(own_c, zp, to_x, x_c), (own_c, zp, to_y, y_c), (own_c, zp, to_a, own_c)]
    hop_a = [(own_c, za, to_p, own_c), (own_c, za, to_x, x_c), (own_c, za, to_y, y_c)]
    hop_b = [(own_c, zb, to_p, own_c), (own_c, zb, to_x, x_c), (own_c, zb, to_y, y_c)]
    diag = [(y_c, z, to_x, diag_c), (x_c, zb, to_y, diag_c)]
    swap = [(diag_c, z, to_p, diag_c), (diag_c, zb, to_p, diag_c)]
    order = own_sends + hop_p + hop_a + hop_b + diag + swap

    def each(up, k, entries, act):
        for entry in entries:
            rel, zz, target, _ = entry
            if target is to_a or (target is to_p and rel == own_c and zz is not z):
                @pl.when(is_mid)
                def _():
                    act(send(up, k, entry))
            else:
                act(send(up, k, entry))

    def start(up, k, entries):
        each(up, k, entries, lambda copy: copy.start())

    def own_local(up, k):
        return pltpu.make_async_copy(slab(up, k, dev, z, True), slab(up, k, dev, z), send_sem.at[lax.rem(k, SRING), len(order)])

    def stage_own(up, k):
        start(up, k, own_sends)
        own_local(up, k).start()

    def stage_1(up, k):
        wait_slab(up, k, own_c, zp)
        start(up, k, hop_p)

        @pl.when(is_mid)
        def _():
            wait_slab(up, k, own_c, za)
            start(up, k, hop_a)

    def stage_2(up, k):
        wait_slab(up, k, own_c, zb)
        start(up, k, hop_b)

    def stage_3(up, k):
        @pl.when(is_end)
        def _():
            wait_slab(up, k, own_c, za)
            start(up, k, hop_a[1:])

    def stage_diag(up, k):
        wait_slab(up, k, y_c, z)
        start(up, k, diag[:1])
        wait_slab(up, k, x_c, zb)
        start(up, k, diag[1:])

    def stage_swap(up, k):
        wait_slab(up, k, diag_c, z)
        start(up, k, swap[:1])
        wait_slab(up, k, diag_c, zb)
        start(up, k, swap[1:])

    def stage_pair(up, k):
        own_local(up, k).wait()
        pair_copy(up, k, own_c, dev).start()
        for zz in (z, zp, za):
            wait_slab(up, k, x_c, zz)
        pair_copy(up, k, x_c, dx).start()
        for zz in (zp, za, zb):
            wait_slab(up, k, y_c, zz)
        pair_copy(up, k, y_c, dy).start()
        for zz in (zp, za):
            wait_slab(up, k, diag_c, zz)
        pair_copy(up, k, diag_c, dd).start()

    def stage_done(up, k):
        for g in range(4):
            pair_copy(up, k, g, pair_cols[g]).wait_recv()

    def stage_sent(up, k):
        each(up, k, order, lambda copy: copy.wait_send())
        for g in range(4):
            pair_copy(up, k, g, cols[g]).wait_send()

    stages = list(zip(OFFSETS[::-1], (stage_sent, stage_done, stage_pair, stage_swap, stage_diag, stage_3, stage_2, stage_1, stage_own)))

    def gather_step(i):
        for offset, stage in stages:
            k = i + offset

            @pl.when(jnp.logical_and(k >= 0, k < TILES))
            def _():
                both(is_up(k), lambda: stage(True, k), lambda: stage(False, k))

    def give_credits():
        for target in (to_p, to_x, to_y, to_c):
            pl.semaphore_signal(credit, inc=1, device_id=target, device_id_type=MESH)

        @pl.when(is_mid)
        def _():
            pl.semaphore_signal(credit, inc=1, device_id=to_a, device_id_type=MESH)

    def wait_credits():
        @pl.when(is_mid)
        def _():
            pl.semaphore_wait(credit, 5)

        @pl.when(is_end)
        def _():
            pl.semaphore_wait(credit, 4)

    quarter = 2 * parity + core

    def back_ref(matrix, layer, slot, sub, part=None):
        c = pl.ds(pl.multiple_of(SUB * sub, SUB), SUB)
        if matrix == 0:
            return back_up.at[layer, slot, :, c] if part is None else back_up.at[layer, slot, pl.ds(*part), c]
        if part is None:
            return back_down.at[layer, slot, c, :]
        return back_down.at[layer, slot, pl.ds(pl.multiple_of(SUB * sub + part[0], 8), part[1]), :]

    def back_copy(matrix, layer, sub, axis):
        part = SPLITS[matrix][axis]
        return remote(back_ref(matrix, layer, 0, sub, part), back_ref(matrix, layer, 2, sub, part), back_send.at[matrix, layer, sub, axis],
                      back_recv.at[matrix, layer, sub, axis], (to_x, to_y, to_p)[axis])

    def send_back(h):
        layer, sub = (LAYERS - 2) - h // (2 * SUBS), lax.rem(h, 2 * SUBS) // 2
        for matrix in range(2):
            @pl.when(lax.rem(h, 2) == matrix)
            def _():
                for axis in range(3):
                    back_copy(matrix, layer, sub, axis).start()

    def swap_own(layer, matrix):
        ref = (back_up, back_down)[matrix]
        return remote(ref.at[layer, 0], ref.at[layer, 1], swap_send.at[matrix, layer, SUBS], swap_recv.at[matrix, layer, SUBS], to_c)

    def swap_sub(matrix, layer, sub):
        return remote(back_ref(matrix, layer, 2, sub), back_ref(matrix, layer, 3, sub), swap_send.at[matrix, layer, sub], swap_recv.at[matrix, layer, sub], to_c)

    def g_copy(layer, stage):
        half = lambda c: pl.ds(pl.multiple_of(G_HALF * c, LANES), G_HALF)
        if stage == 0:
            src, dst, target = send_g.at[layer, :, half(1 - core)], recv_first.at[layer], to_c
        elif stage == 5:
            src, dst, target = half_g.at[layer, 4], recv_last.at[layer], to_c
        else:
            src, dst, target = half_g.at[layer, stage - 1], recv_half.at[layer, stage - 1], (to_x, to_y, to_p, to_b)[stage - 1]
        return remote(src, dst, g_send.at[layer, stage], g_recv.at[layer, stage], target)

    def g_step(layer, stage):
        if stage > 0:
            g_copy(layer, stage - 1).wait()
        if stage == 1:
            half_g[layer, 0] = send_g[layer, :, pl.ds(pl.multiple_of(G_HALF * core, LANES), G_HALF)] + recv_first[layer]
        elif 1 < stage < 6:
            half_g[layer, stage - 1] = half_g[layer, stage - 2] + recv_half[layer, stage - 2]
        if stage < 6:
            g_copy(layer, stage).start()

    def g_finish(layer):
        send_g[layer, :, pl.ds(pl.multiple_of(G_HALF * core, LANES), G_HALF)] = half_g[layer, 4]
        send_g[layer, :, pl.ds(pl.multiple_of(G_HALF * (1 - core), LANES), G_HALF)] = recv_last[layer]
        total = send_g[layer]
        grad_b[layer, :, 0:G_EDGE] = total[0:RANK, 0:G_EDGE]
        grad_b[layer, :, G_EDGE:FF] = total[RANK:2 * RANK, 0:FF - G_EDGE]
        grad_a[layer, :, :] = total[RANK:2 * RANK, FF - G_EDGE:G_EDGE]

    def write_blocks(ref, blocks):
        for i in range(3):
            ref[16 * i:16 * i + 16, :] = jnp.concatenate([blocks[2 * i], blocks[2 * i + 1]], axis=0).astype(BF16)

    def rows8(value):
        return jnp.concatenate([value, jnp.zeros_like(value)], axis=0)

    def adapters(layer):
        for c in range(0, FF, HIDDEN):
            write_blocks(b6.at[:, c:c + HIDDEN], stack_right(rows8(adapt_b[layer, :, c:c + HIDDEN])))
        write_blocks(a6, stack_right(rows8(adapt_a[layer])))

    def normalize(layer, save):
        @pl.loop(0, TOKENS // LANES)
        def _(i):
            r = pl.ds(pl.multiple_of(i * LANES, LANES), LANES)
            xf = x[r, :].astype(F32)
            inv = lax.rsqrt(jnp.mean(xf * xf, axis=-1, keepdims=True) + NORM_EPS)
            u[r, :] = (xf * inv).astype(BF16)
            inv_s[layer, r, :] = jnp.broadcast_to(inv, (LANES, LANES))

        adapters(layer)
        low = sum3(dot_t(a6[0:32, :], u[...]))
        left = stack_left(low)
        v3[layer, :, :] = jnp.concatenate([left[0], left[3], left[5]], axis=0)
        wide = jnp.concatenate(list(left) + [jnp.zeros((80, TOKENS), F32)], axis=0)
        v6[...] = jnp.transpose(wide).astype(BF16)
        if save:
            save_x(layer).start()
            save_u(layer).start()

    def save_x(layer):
        return pltpu.make_async_copy(x, resids.at[layer], load_sem.at[4])

    def save_u(layer):
        return pltpu.make_async_copy(u, normeds.at[layer], load_sem.at[5])

    def first_load(layer, t, buf):
        return pltpu.make_async_copy(land_up.at[lax.rem(layer, 2), :, pl.ds(pl.multiple_of(UP_TILE * t, LANES), UP_TILE)], buf.at[lax.rem(t, 2)], w_sem.at[0, lax.rem(t, 2)])

    def act_store(layer, t, acts):
        return pltpu.make_async_copy(acts.at[lax.rem(t, 2)], pre_acts.at[layer, :, pl.ds(pl.multiple_of(UP_TILE * t, LANES), UP_TILE)], act_sem.at[lax.rem(t, 2)])

    def keep_half(layer, t, h, buf):
        block = 2 * t + h - 5 * quarter
        copy = pltpu.make_async_copy(buf.at[lax.rem(t, 2), :, 256 * h:256 * h + 256],
                                     back_up.at[layer, 0, :, pl.ds(pl.multiple_of(256 * jnp.clip(block, 0, 4), LANES), 256)], keep_sem.at[h])
        return jnp.logical_and(block >= 0, block < 5), copy

    def first_product(layer, t, buf, acts, s):
        first_load(layer, t, buf).wait()
        for h in range(2):
            cond, copy = keep_half(layer, t, h, buf)
            pl.when(cond)(copy.start)

        @pl.when(t >= 2)
        def _():
            act_store(layer, t - 2, acts).wait()

        c = pl.ds(pl.multiple_of(UP_TILE * t, LANES), UP_TILE)
        pre = dot(u[...], buf[lax.rem(t, 2)]) + dot(v6[...], b6[:, c])
        act = pre.astype(BF16)
        acts[lax.rem(t, 2)] = act
        af = act.astype(F32)
        _, th = gelu_inner(af)
        half = 0.5 * af
        s[:, c] = (half + half * th).astype(BF16)
        act_store(layer, t, acts).start()
        for h in range(2):
            cond, copy = keep_half(layer, t, h, buf)
            pl.when(cond)(copy.wait)

    def second_load(layer, c, buf):
        return pltpu.make_async_copy(land_down.at[lax.rem(layer, 2), :, pl.ds(pl.multiple_of(OUT_COLS * c, LANES), OUT_COLS)], buf.at[lax.rem(c, 2)], w_sem.at[1, lax.rem(c, 2)])

    def second_keep(layer, c, buf):
        cc = pl.ds(pl.multiple_of(OUT_COLS * c, LANES), OUT_COLS)
        return pltpu.make_async_copy(buf.at[lax.rem(c, 2), pl.ds(pl.multiple_of(QUARTER * quarter, 16), QUARTER), :], back_down.at[layer, 0, :, cc], keep_sem.at[2])

    def second_product(layer, c, buf, s):
        second_load(layer, c, buf).wait()
        keep = second_keep(layer, c, buf)
        keep.start()
        cc = pl.ds(pl.multiple_of(OUT_COLS * c, LANES), OUT_COLS)
        x[:, cc] = (x[:, cc].astype(F32) + dot(s[...], buf[lax.rem(c, 2)])).astype(BF16)
        keep.wait()

    def gelu_both(act):
        af = act.astype(F32)
        x2, th = gelu_inner(af)
        half = 0.5 * af
        slope = 0.5 + 0.5 * th + half * (1.0 - th * th) * (GELU_S + (3.0 * GELU_S * GELU_C) * x2)
        return half + half * th, slope

    def low_parts(layer, dpre, c):
        cc = pl.ds(c, dpre.shape[1])
        dlow[...] += sum3(dot_t(b6[0:32, cc], dpre))
        gb[:, cc] = sum3(dot(v3[layer].astype(BF16), dpre))

    def close_layer(layer, acc):
        left = stack_left(dlow[...])
        wide = jnp.concatenate(list(left) + [jnp.zeros((80, TOKENS), F32)], axis=0)
        v6[...] = jnp.transpose(wide).astype(BF16)
        narrow = jnp.concatenate([left[0], left[3], left[5]], axis=0).astype(BF16)
        ga = sum3(dot(narrow, u[...]))
        send_g[layer, 0:RANK, 0:G_EDGE] = gb[0:RANK, 0:G_EDGE]
        send_g[layer, RANK:2 * RANK, 0:FF - G_EDGE] = gb[0:RANK, G_EDGE:FF]
        send_g[layer, RANK:2 * RANK, FF - G_EDGE:G_EDGE] = ga[0:RANK]
        send_g[layer, :, G_EDGE:G_COLS] = jnp.zeros((8, G_COLS - G_EDGE), F32)
        g_step(layer, 0)

        @pl.loop(0, TOKENS // LANES)
        def _(i):
            r = pl.ds(pl.multiple_of(i * LANES, LANES), LANES)
            side = dot(v6[r, :], a6[...]).astype(BF16)
            dn = (acc[r, :].astype(BF16) + side).astype(F32)
            xf = x[r, :].astype(F32)
            inv = inv_s[layer, r, 0:1]
            row = jnp.mean(xf * dn, axis=-1, keepdims=True)
            d[r, :] = (d[r, :].astype(F32) + inv * dn - xf * (inv * inv * inv * row)).astype(BF16)

    zero128 = jnp.zeros((80, HIDDEN), BF16)
    a6[48:LANES, :] = zero128
    for c in range(0, FF, HIDDEN):
        b6[48:LANES, c:c + HIDDEN] = zero128

    def forward(buf_a, buf_b, s, acts):
        def iteration(j, carry):
            i = j - LEAD

            pl.when(i == 2 * 2 * NT - LEAD)(wait_credits)
            gather_step(i)

            @pl.when(i == -2)
            def _():
                loads[2].wait()
                normalize(0, True)

            second = i >= 2 * NT + 4
            layer = jnp.where(second, 1, 0)
            lo = jnp.where(second, 2 * NT + 5, 1)

            @pl.when(jnp.logical_and(i >= lo - 1, i < lo - 1 + NT))
            def _():
                first_load(layer, i - lo + 1, buf_a).start()

            @pl.when(jnp.logical_and(i >= lo, i < lo + NT))
            def _():
                first_product(layer, i - lo, buf_a, acts, s)

            @pl.when(i == lo + NT)
            def _():
                act_store(layer, NT - 2, acts).wait()
                act_store(layer, NT - 1, acts).wait()

            pieces = HIDDEN // OUT_COLS
            prev = jnp.where(i >= 4 * NT - 1, 1, 0)
            lo2 = 2 * NT + 2 * NT * prev

            @pl.when(jnp.logical_and(i >= lo2 - 1, i < lo2 - 1 + pieces))
            def _():
                second_load(prev, i - lo2 + 1, buf_b).start()

            @pl.when(i == lo2)
            def _():
                save_x(prev).wait()
                save_u(prev).wait()

            @pl.when(jnp.logical_and(i >= lo2, i < lo2 + pieces))
            def _():
                second_product(prev, i - lo2, buf_b, s)

            @pl.when(i == 2 * NT + pieces - 1)
            def _():
                give_credits()
                normalize(1, True)

            @pl.when(i == 4 * NT + pieces - 1)
            def _():
                normalize(2, False)
            return carry

        lax.fori_loop(0, FUSED_FROM + LEAD, iteration, 0)

    pl.run_scoped(
        forward,
        pltpu.VMEM((2, HIDDEN, UP_TILE), BF16), pltpu.VMEM((2, FF, OUT_COLS), BF16),
        pltpu.VMEM((TOKENS, FF), BF16), pltpu.VMEM((2, TOKENS, UP_TILE), BF16),
    )

    loads[3].wait()

    last = LAYERS - 1

    def fused_loads(t, buf_a, buf_b):
        return (first_load(last, t, buf_a),
                pltpu.make_async_copy(land_down.at[last % 2, pl.ds(pl.multiple_of(UP_TILE * t, 16), UP_TILE), :], buf_b.at[lax.rem(t, 2)], w_sem.at[1, lax.rem(t, 2)]))

    def fused(buf_a, buf_b, dpre, y, acc, out):
        y[...] = jnp.zeros_like(y)
        acc[...] = jnp.zeros_like(acc)
        dlow[...] = jnp.zeros_like(dlow)
        for matrix in range(2):
            swap_own(LAYERS - 2, matrix).start()

        def iteration(i, carry):
            gather_step(i)
            n = i - FUSED_FROM
            send_back(n)

            @pl.when(n < NT)
            def _():
                for load in fused_loads(n, buf_a, buf_b):
                    load.start()

            @pl.when(n >= 1)
            def _():
                t = n - 1
                slot = lax.rem(t, 2)
                for load in fused_loads(t, buf_a, buf_b):
                    load.wait()
                c = pl.multiple_of(UP_TILE * t, LANES)

                for h in range(TOKENS // ROWS):
                    r = slice(ROWS * h, ROWS * h + ROWS)
                    pre = dot(u[r, :], buf_a[slot]) + dot(v6[r, :], b6[:, pl.ds(c, UP_TILE)])
                    dh = dot_t(d[r, :], buf_b[slot]).astype(BF16).astype(F32)
                    s, slope = gelu_both(pre.astype(BF16))
                    dp = (dh * slope).astype(BF16)
                    dpre[r, :] = dp
                    y[r, :] += dot(s.astype(BF16), buf_b[slot])
                    acc[r, :] += dot_t(dp, buf_a[slot])

                low_parts(last, dpre[...], c)
            return carry

        lax.fori_loop(FUSED_FROM, TILES + 1, iteration, 0)

        pl.loop(TILES + 1 - FUSED_FROM, 4 * SUBS)(send_back)

        @pl.loop(0, TOKENS // LANES)
        def _(i):
            r = pl.ds(pl.multiple_of(i * LANES, LANES), LANES)
            out[r, :] = (x[r, :].astype(F32) + y[r, :]).astype(BF16)

        out_copy = pltpu.make_async_copy(out, out_tokens, load_sem.at[6])
        out_copy.start()
        close_layer(last, acc)
        out_copy.wait()

    pl.run_scoped(
        fused,
        pltpu.VMEM((2, HIDDEN, UP_TILE), BF16), pltpu.VMEM((2, UP_TILE, HIDDEN), BF16), pltpu.VMEM((TOKENS, UP_TILE), BF16),
        pltpu.VMEM((TOKENS, HIDDEN), F32), pltpu.VMEM((TOKENS, HIDDEN), F32), pltpu.VMEM((TOKENS, HIDDEN), BF16),
    )

    steps = 2 * SUBS

    def backward(buf_a, buf_b, act, dpre, acc):
        def place(n):
            layer, b = (LAYERS - 2) - n // steps, lax.rem(n, steps)
            outside, sub = b // SUBS, lax.rem(b, SUBS)
            base = 2 * (parity + outside - 2 * parity * outside)
            return layer, b, outside, sub, [pl.multiple_of(QUARTER * (base + c) + SUB * sub, SUB) for c in (core, 1 - core)]

        def loads_of(n):
            layer, _, outside, sub, fs = place(n)
            s = lax.rem(n, 2)
            copies = []
            for i in range(2):
                half = pl.ds(SUB * i, SUB)
                copies += [(back_ref(0, layer, 2 * outside + i, sub), buf_a.at[s, :, half]), (back_ref(1, layer, 2 * outside + i, sub), buf_b.at[s, half, :]),
                           (pre_acts.at[layer, :, pl.ds(fs[i], SUB)], act.at[s, :, half])]
            return [pltpu.make_async_copy(src, dst, back_sem.at[s, i]) for i, (src, dst) in enumerate(copies)]

        def pass_on(n):
            layer, _, outside, sub, _ = place(n)

            @pl.when(jnp.logical_and(n < 2 * steps, outside == 1))
            def _():
                for matrix in range(2):
                    for axis in range(3):
                        back_copy(matrix, layer, sub, axis).wait_recv()
                    swap_sub(matrix, layer, sub).start()

        def fetch(n):
            layer, b, outside, sub, _ = place(n)

            @pl.when(b == 0)
            def _():
                for matrix in range(2):
                    swap_own(layer, matrix).wait_recv()

            @pl.when(outside == 1)
            def _():
                for matrix in range(2):
                    swap_sub(matrix, layer, sub).wait_recv()

            for load in loads_of(n):
                load.start()

        def reloads(layer):
            return (pltpu.make_async_copy(resids.at[layer], x, load_sem.at[4]), pltpu.make_async_copy(normeds.at[layer], u, load_sem.at[5]))

        for matrix in range(2):
            swap_own(0, matrix).start()
        fetch(0)

        def iteration(n, carry):
            layer, b, _, _, fs = place(n)
            s = lax.rem(n, 2)

            @pl.when(b == 0)
            def _():
                for load in reloads(layer):
                    load.start()
                adapters(layer)
                acc[...] = jnp.zeros_like(acc)
                dlow[...] = jnp.zeros_like(dlow)

            for stage in range(1, G_STAGES + 1):
                @pl.when(n == steps + 2 + stage)
                def _():
                    for done in range(1, LAYERS):
                        g_step(done, stage)
            for load in loads_of(n):
                load.wait()
            pass_on(n + 2)
            pl.when(n + 1 < 2 * steps)(lambda: fetch(n + 1))
            for h in range(TOKENS // ROWS):
                r = slice(ROWS * h, ROWS * h + ROWS)
                dh = dot_t(d[r, :], buf_b[s]).astype(BF16).astype(F32)
                _, slope = gelu_both(act[s, r, :])
                dp = (dh * slope).astype(BF16)
                dpre[r, :] = dp
                acc[r, :] += dot_t(dp, buf_a[s])
            for i in range(2):
                low_parts(layer, dpre[:, SUB * i:SUB * i + SUB], fs[i])

            @pl.when(b == steps - 1)
            def _():
                for load in reloads(layer):
                    load.wait()
                close_layer(layer, acc)
            return carry

        lax.fori_loop(0, 2 * steps, iteration, 0)
        grad_copy = pltpu.make_async_copy(d, grad_tokens, load_sem.at[6])
        grad_copy.start()
        for stage in range(1, G_STAGES + 1):
            g_step(0, stage)
        pl.loop(0, LAYERS)(g_finish)
        grad_copy.wait()

    pl.run_scoped(
        backward,
        pltpu.VMEM((2, HIDDEN, 2 * SUB), BF16), pltpu.VMEM((2, 2 * SUB, HIDDEN), BF16), pltpu.VMEM((2, TOKENS, 2 * SUB), BF16),
        pltpu.VMEM((TOKENS, 2 * SUB), BF16), pltpu.VMEM((TOKENS, HIDDEN), F32),
    )

    @pl.loop(0, LAYERS - 1)
    def _(layer):
        for matrix in range(2):
            swap_own(layer, matrix).wait_send()

            @pl.loop(0, SUBS)
            def _(sub):
                swap_sub(matrix, layer, sub).wait_send()
                for axis in range(3):
                    back_copy(matrix, layer, sub, axis).wait_send()


def step(tokens, cotangent, w_up, w_down, adapt_a, adapt_b):
    any_spec, vmem = pl.BlockSpec(memory_space=pl.ANY), pl.BlockSpec(memory_space=pltpu.VMEM)
    sds = jax.ShapeDtypeStruct
    dma = pltpu.SemaphoreType.DMA
    outs = [
        (sds((TOKENS, HIDDEN), BF16), any_spec), (sds((TOKENS, HIDDEN), BF16), any_spec),
        (sds((LAYERS, RANK, HIDDEN), F32), vmem), (sds((LAYERS, RANK, FF), F32), vmem),
        (sds((2, HIDDEN, FF), BF16), any_spec), (sds((2, FF, HIDDEN), BF16), any_spec),
        (sds((2, 4, HIDDEN, QUARTER), BF16), any_spec), (sds((2, 4, QUARTER, HIDDEN), BF16), any_spec),
        (sds((2, TOKENS, FF), BF16), any_spec), (sds((2, TOKENS, HIDDEN), BF16), any_spec), (sds((2, TOKENS, HIDDEN), BF16), any_spec),
    ]
    result = pl.pallas_call(
        step_kernel,
        out_shape=[o[0] for o in outs],
        in_specs=[any_spec] * 4 + [vmem] * 2,
        out_specs=[o[1] for o in outs],
        scratch_shapes=[
            pltpu.VMEM((LAYERS, UP_ROWS, FF), BF16), pltpu.VMEM((LAYERS, DOWN_ROWS, HIDDEN), BF16),
            pltpu.VMEM((TOKENS, HIDDEN), BF16), pltpu.VMEM((TOKENS, HIDDEN), BF16), pltpu.VMEM((TOKENS, HIDDEN), BF16),
            pltpu.VMEM((LAYERS, TOKENS, LANES), F32), pltpu.VMEM((LANES, FF), BF16), pltpu.VMEM((LANES, HIDDEN), BF16),
            pltpu.VMEM((TOKENS, LANES), BF16), pltpu.VMEM((LAYERS, 24, TOKENS), F32), pltpu.VMEM((8, TOKENS), F32), pltpu.VMEM((8, FF), F32),
            pltpu.VMEM((LAYERS, 8, G_COLS), F32), pltpu.VMEM((LAYERS, 5, 8, G_HALF), F32), pltpu.VMEM((LAYERS, 8, G_HALF), F32),
            pltpu.VMEM((LAYERS, 4, 8, G_HALF), F32), pltpu.VMEM((LAYERS, 8, G_HALF), F32),
            dma((RING, 16)), dma((RING, 4)), dma((SRING, 22)), dma((2, 2, SUBS, 3)), dma((2, 2, SUBS, 3)), dma((2, 2, SUBS + 1)), dma((2, 2, SUBS + 1)),
            dma((LAYERS, G_STAGES)), dma((LAYERS, G_STAGES)), dma((7,)), dma((2, 6)), dma((2, 2)), dma((2,)), dma((3,)), pltpu.SemaphoreType.REGULAR,
        ],
        compiler_params=pltpu.CompilerParams(collective_id=0, has_side_effects=True, vmem_limit_bytes=67_000_000),
        cost_estimate=pl.CostEstimate(flops=12 * 2 * TOKENS * HIDDEN * FF, bytes_accessed=400_000_000, transcendentals=0),
        name="mlp_stack",
    )(tokens, cotangent, w_up, w_down, jnp.swapaxes(adapt_a, 1, 2), adapt_b)
    return result[0], result[1], jnp.swapaxes(result[2], 1, 2), result[3]


def solution(mesh):
    tok_spec, weight_spec = P(GROUP, None), P(None, GROUP, None)
    return jax.shard_map(step, mesh=mesh, in_specs=(tok_spec, tok_spec, weight_spec, weight_spec, P(), P()), out_specs=(tok_spec, tok_spec, P(), P()), check_vma=False)
```

```python
import math

import jax
import jax.numpy as jnp
from jax import lax
from jax.experimental import pallas as pl
from jax.experimental.pallas import tpu as pltpu
from jax.sharding import PartitionSpec as P

GROUP = ("data", "local")
MESH = pl.DeviceIdType.MESH
BF16, F32 = jnp.bfloat16, jnp.float32
ROWS = 512
LANES = 128
NORM_EPS = 1e-6
GELU_S = math.sqrt(2.0 / math.pi)
GELU_C = 0.044715

LAYERS, TOKENS, HIDDEN, FF, RANK = 3, 1024, 1280, 5120, 4
NT = 10
TILES = 2 * LAYERS * NT
UP_ROWS, DOWN_ROWS = HIDDEN // 32, FF // 32
UP_TILE, DOWN_TILE = FF // NT, DOWN_ROWS // NT
OUT_COLS = 256
QUARTER = FF // 4
RING, SRING = 28, 16
OFFSETS = (7, 6, 5, 4, 3, 2, 1, 0, -1)
LEAD = OFFSETS[0]
FAR_LEAD = 2 * LEAD - 1
MIX = 4 * NT
FUSED_FROM = MIX + HIDDEN // OUT_COLS
FUSED_TO = FUSED_FROM + 2 * NT - 2
BACK_FROM = 48
BACK_EARLY, BACK_EVERY = 3, 3
BACK_STEADY = BACK_FROM + BACK_EVERY * BACK_EARLY - 1
BACK_SENT = BACK_EARLY + FUSED_TO - BACK_STEADY
BACK_AHEAD = 2
SUMS_FROM = 14
SUB = 256
SUBS = QUARTER // SUB
G_COLS = 3328
G_HALF = G_COLS // 2
G_EDGE = (FF + HIDDEN) // 2
G_STAGES = 6
SPLITS = (((0, 424), (424, 424), (848, 432)), ((0, 88), (88, 88), (176, 80)))


def dot(a, b):
    return jnp.dot(a, b, preferred_element_type=F32)


def dot_t(a, b):
    return lax.dot_general(a, b, (((1,), (1,)), ((), ())), preferred_element_type=F32)


def split3(x):
    hi = x.astype(BF16).astype(F32)
    rest = x - hi
    mid = rest.astype(BF16).astype(F32)
    return hi, mid, (rest - mid).astype(BF16).astype(F32)


def stack_left(x):
    hi, mid, lo = split3(x)
    return hi, hi, hi, mid, mid, lo


def stack_right(x):
    hi, mid, lo = split3(x)
    return hi, mid, lo, hi, mid, hi


def sum3(x):
    return x[0:8] + x[8:16] + x[16:24]


def gelu_inner(x):
    x2 = x * x
    return x2, jnp.tanh(x * (GELU_S + (GELU_S * GELU_C) * x2))


def step_kernel(
    tokens, cotangent, w_up, w_down, adapt_a, adapt_b,
    out_tokens, grad_tokens, grad_a, grad_b,
    land_up, land_down, back_up, back_down, slopes, resids, normeds,
    own_up, own_down, x, u, d, inv_s, b6, a6, v6, v3, perm, dlow, gb, send_g, half_g, recv_first, recv_half, recv_last,
    recv_sem, pair_sem, send_sem, back_recv, back_send, swap_recv, swap_send, g_recv, g_send, load_sem, back_sem, w_sem, act_sem, keep_sem, credit,
):
    z = lax.axis_index("local")
    dev = lax.axis_index("data")
    core = lax.rem(dev, 2)
    dx = dev + 2 - 4 * lax.rem(dev // 2, 2)
    dy = dev + 4 - 8 * (dev // 4)
    dd = dx + dy - dev
    dc = dev + 1 - 2 * core
    zp = z + 1 - 2 * lax.rem(z, 2)
    za, zb = 3 - z, 3 - zp
    parity = lax.rem(lax.rem(dev // 2, 2) + dev // 4 + z, 2)
    is_end = jnp.logical_or(z == 0, z == 3)
    is_mid = jnp.logical_not(is_end)
    to_p, to_a, to_b = (zp, dev), (za, dev), (zb, dev)
    to_x, to_y, to_c = (z, dx), (z, dy), (z, dc)
    cols = (dev, dx, dy, dd)
    pair_cols = (dc, dc + dx - dev, dc + dy - dev, dc + dd - dev)

    def remote(src, dst, ssem, rsem, target):
        return pltpu.make_async_remote_copy(src, dst, ssem, rsem, device_id=target, device_id_type=MESH)

    def both(cond, on, off):
        pl.when(cond)(on)
        pl.when(jnp.logical_not(cond))(off)

    loads = [
        pltpu.make_async_copy(w_up, own_up, load_sem.at[0]),
        pltpu.make_async_copy(w_down, own_down, load_sem.at[1]),
        pltpu.make_async_copy(tokens, x, load_sem.at[2]),
        pltpu.make_async_copy(cotangent, d, load_sem.at[3]),
    ]
    for load in loads:
        load.start()
    barrier = pltpu.get_barrier_semaphore()
    for target in (to_p, to_x, to_y, to_c, to_b):
        pl.semaphore_signal(barrier, inc=1, device_id=target, device_id_type=MESH)

    @pl.when(is_mid)
    def _():
        pl.semaphore_signal(barrier, inc=1, device_id=to_a, device_id_type=MESH)
        pl.semaphore_wait(barrier, 6)

    @pl.when(is_end)
    def _():
        pl.semaphore_wait(barrier, 5)

    loads[0].wait()
    loads[1].wait()

    def is_up(k):
        return jnp.where(k < MIX, lax.rem(k // NT, 2) == 0, lax.rem(k, 2) == 1)

    def tile_of(k):
        return jnp.where(k < MIX, lax.rem(k, NT), (k - MIX) // 2)

    def slab(up, k, col, zz, own=False):
        layer, t, n = k // (2 * NT), tile_of(k), 4 * col + zz
        slot = lax.rem(layer, 2)
        if up:
            c = pl.ds(pl.multiple_of(UP_TILE * t, LANES), UP_TILE)
            return own_up.at[layer, :, c] if own else land_up.at[slot, pl.ds(pl.multiple_of(UP_ROWS * n, 8), UP_ROWS), c]
        r = pl.multiple_of(DOWN_TILE * t, 16)
        return own_down.at[layer, pl.ds(r, DOWN_TILE), :] if own else land_down.at[slot, pl.ds(pl.multiple_of(DOWN_ROWS * n + r, 16), DOWN_TILE), :]

    def send(up, k, entry):
        rel, zz, target, to_rel = entry
        own = rel == own_c and zz is z
        index = [e is entry for e in order].index(True)
        return remote(slab(up, k, cols[rel], zz, own), slab(up, k, cols[rel], zz), send_sem.at[lax.rem(k, SRING), index],
                      recv_sem.at[lax.rem(k, RING), to_rel * 4 + zz], target)

    def wait_slab(up, k, rel, zz):
        s = slab(up, k, cols[rel], zz)
        remote(s, s, send_sem.at[0, 0], recv_sem.at[lax.rem(k, RING), rel * 4 + zz], to_x).wait_recv()

    def pair_copy(up, k, g, c):
        layer, t = k // (2 * NT), tile_of(k)
        slot = lax.rem(layer, 2)
        if up:
            s = land_up.at[slot, pl.ds(pl.multiple_of(4 * UP_ROWS * c, 8), 4 * UP_ROWS), pl.ds(pl.multiple_of(UP_TILE * t, LANES), UP_TILE)]
        else:
            s = land_down.reshape(2, 32, DOWN_ROWS, HIDDEN).at[slot, pl.ds(4 * c, 4), pl.ds(pl.multiple_of(DOWN_TILE * t, 16), DOWN_TILE), :]
        return remote(s, s, send_sem.at[lax.rem(k, SRING), len(order) + 1 + g], pair_sem.at[lax.rem(k, RING), g], to_c)

    own_c, x_c, y_c, diag_c = range(4)
    own_sends = [(own_c, z, to_p, own_c), (own_c, z, to_a, own_c), (own_c, z, to_x, x_c), (own_c, z, to_y, y_c)]
    hop_p = [(own_c, zp, to_x, x_c), (own_c, zp, to_y, y_c), (own_c, zp, to_a, own_c)]
    hop_a = [(own_c, za, to_p, own_c), (own_c, za, to_x, x_c), (own_c, za, to_y, y_c)]
    hop_b = [(own_c, zb, to_p, own_c), (own_c, zb, to_x, x_c), (own_c, zb, to_y, y_c)]
    diag = [(y_c, z, to_x, diag_c), (x_c, zb, to_y, diag_c)]
    swap = [(diag_c, z, to_p, diag_c), (diag_c, zb, to_p, diag_c)]
    order = own_sends + hop_p + hop_a + hop_b + diag + swap

    def each(up, k, entries, act):
        for entry in entries:
            rel, zz, target, _ = entry
            if target is to_a or (target is to_p and rel == own_c and zz is not z):
                @pl.when(is_mid)
                def _():
                    act(send(up, k, entry))
            else:
                act(send(up, k, entry))

    def start(up, k, entries):
        each(up, k, entries, lambda copy: copy.start())

    def own_local(up, k):
        return pltpu.make_async_copy(slab(up, k, dev, z, True), slab(up, k, dev, z), send_sem.at[lax.rem(k, SRING), len(order)])

    def stage_own(up, k):
        start(up, k, own_sends)
        own_local(up, k).start()

    def stage_1(up, k):
        wait_slab(up, k, own_c, zp)
        start(up, k, hop_p)

        @pl.when(is_mid)
        def _():
            wait_slab(up, k, own_c, za)
            start(up, k, hop_a)

    def stage_2(up, k):
        wait_slab(up, k, own_c, zb)
        start(up, k, hop_b)

    def stage_3(up, k):
        @pl.when(is_end)
        def _():
            wait_slab(up, k, own_c, za)
            start(up, k, hop_a[1:])

    def stage_diag(up, k):
        wait_slab(up, k, y_c, z)
        start(up, k, diag[:1])
        wait_slab(up, k, x_c, zb)
        start(up, k, diag[1:])

    def stage_swap(up, k):
        wait_slab(up, k, diag_c, z)
        start(up, k, swap[:1])
        wait_slab(up, k, diag_c, zb)
        start(up, k, swap[1:])

    def stage_pair(up, k):
        own_local(up, k).wait()
        pair_copy(up, k, own_c, dev).start()
        for zz in (z, zp, za):
            wait_slab(up, k, x_c, zz)
        pair_copy(up, k, x_c, dx).start()
        for zz in (zp, za, zb):
            wait_slab(up, k, y_c, zz)
        pair_copy(up, k, y_c, dy).start()
        for zz in (zp, za):
            wait_slab(up, k, diag_c, zz)
        pair_copy(up, k, diag_c, dd).start()

    def stage_done(up, k):
        for g in range(4):
            pair_copy(up, k, g, pair_cols[g]).wait_recv()

    def stage_sent(up, k):
        each(up, k, order, lambda copy: copy.wait_send())
        for g in range(4):
            pair_copy(up, k, g, cols[g]).wait_send()

    stages = list(zip(OFFSETS[:0:-1], (stage_sent, stage_done, stage_pair, stage_swap, stage_diag, stage_3, stage_2, stage_1)))

    def at_tile(k, stage):
        @pl.when(jnp.logical_and(k >= 0, k < TILES))
        def _():
            both(is_up(k), lambda: stage(True, k), lambda: stage(False, k))

    def gather_step(i):
        for offset, stage in stages:
            at_tile(i + offset, stage)
        first = jnp.minimum(2 * (i + LEAD), i + FAR_LEAD)

        @pl.loop(first, jnp.minimum(2 * (i + LEAD) + 2, i + FAR_LEAD + 1))
        def _(k):
            at_tile(k, stage_own)

    def give_credits():
        for target in (to_p, to_x, to_y, to_c):
            pl.semaphore_signal(credit, inc=1, device_id=target, device_id_type=MESH)

        @pl.when(is_mid)
        def _():
            pl.semaphore_signal(credit, inc=1, device_id=to_a, device_id_type=MESH)

    def wait_credits():
        @pl.when(is_mid)
        def _():
            pl.semaphore_wait(credit, 5)

        @pl.when(is_end)
        def _():
            pl.semaphore_wait(credit, 4)

    quarter = 2 * parity + core

    def back_ref(matrix, layer, slot, sub, part=None):
        c = pl.ds(pl.multiple_of(SUB * sub, SUB), SUB)
        if matrix == 0:
            return back_up.at[layer, slot, :, c] if part is None else back_up.at[layer, slot, pl.ds(*part), c]
        if part is None:
            return back_down.at[layer, slot, c, :]
        return back_down.at[layer, slot, pl.ds(pl.multiple_of(SUB * sub + part[0], 8), part[1]), :]

    def back_copy(matrix, layer, sub, axis):
        part = SPLITS[matrix][axis]
        return remote(back_ref(matrix, layer, 0, sub, part), back_ref(matrix, layer, 2, sub, part), back_send.at[matrix, layer, sub, axis],
                      back_recv.at[matrix, layer, sub, axis], (to_x, to_y, to_p)[axis])

    def send_back(h):
        layer, sub = (LAYERS - 2) - h // (2 * SUBS), lax.rem(h, 2 * SUBS) // 2
        for matrix in range(2):
            @pl.when(lax.rem(h, 2) == matrix)
            def _():
                for axis in range(3):
                    back_copy(matrix, layer, sub, axis).start()

    def swap_own(layer, matrix):
        ref = (back_up, back_down)[matrix]
        return remote(ref.at[layer, 0], ref.at[layer, 1], swap_send.at[matrix, layer, SUBS], swap_recv.at[matrix, layer, SUBS], to_c)

    def swap_sub(matrix, layer, sub):
        return remote(back_ref(matrix, layer, 2, sub), back_ref(matrix, layer, 3, sub), swap_send.at[matrix, layer, sub], swap_recv.at[matrix, layer, sub], to_c)

    def g_copy(layer, stage):
        half = lambda c: pl.ds(pl.multiple_of(G_HALF * c, LANES), G_HALF)
        if stage == 0:
            src, dst, target = send_g.at[layer, :, half(1 - core)], recv_first.at[layer], to_c
        elif stage == 5:
            src, dst, target = half_g.at[layer, 4], recv_last.at[layer], to_c
        else:
            src, dst, target = half_g.at[layer, stage - 1], recv_half.at[layer, stage - 1], (to_x, to_y, to_p, to_b)[stage - 1]
        return remote(src, dst, g_send.at[layer, stage], g_recv.at[layer, stage], target)

    def g_step(layer, stage):
        if stage > 0:
            g_copy(layer, stage - 1).wait()
        if stage == 1:
            half_g[layer, 0] = send_g[layer, :, pl.ds(pl.multiple_of(G_HALF * core, LANES), G_HALF)] + recv_first[layer]
        elif 1 < stage < 6:
            half_g[layer, stage - 1] = half_g[layer, stage - 2] + recv_half[layer, stage - 2]
        if stage < 6:
            g_copy(layer, stage).start()

    def g_finish(layer):
        send_g[layer, :, pl.ds(pl.multiple_of(G_HALF * core, LANES), G_HALF)] = half_g[layer, 4]
        send_g[layer, :, pl.ds(pl.multiple_of(G_HALF * (1 - core), LANES), G_HALF)] = recv_last[layer]
        total = send_g[layer]
        grad_b[layer, :, 0:G_EDGE] = total[0:RANK, 0:G_EDGE]
        grad_b[layer, :, G_EDGE:FF] = total[RANK:2 * RANK, 0:FF - G_EDGE]
        grad_a[layer, :, :] = total[RANK:2 * RANK, FF - G_EDGE:G_EDGE]

    def write_blocks(ref, blocks):
        for i in range(3):
            ref[16 * i:16 * i + 16, :] = jnp.concatenate([blocks[2 * i], blocks[2 * i + 1]], axis=0).astype(BF16)

    def rows8(value):
        return jnp.concatenate([value, jnp.zeros_like(value)], axis=0)

    def build_order():
        @pl.loop(0, HIDDEN // OUT_COLS)
        def _(block):
            o = lax.broadcasted_iota(jnp.int32, (HIDDEN, OUT_COLS), 1) + OUT_COLS * block
            c = lax.broadcasted_iota(jnp.int32, (HIDDEN, OUT_COLS), 0)
            tile, place = o // LANES, o % LANES
            source = DOWN_ROWS * (place // DOWN_TILE) + DOWN_TILE * tile + place % DOWN_TILE
            perm[:, pl.ds(pl.multiple_of(OUT_COLS * block, OUT_COLS), OUT_COLS)] = jnp.where(c == source, 1.0, 0.0).astype(BF16)

        parts = FF // HIDDEN
        moved = [dot(own_up[LAYERS - 1, :, HIDDEN * m:HIDDEN * m + HIDDEN], perm[...]).astype(BF16) for m in range(parts)]
        for m in range(parts):
            for tile in range(NT):
                first = UP_TILE * tile + LANES * m
                own_up[LAYERS - 1, :, first:first + LANES] = moved[m][:, LANES * tile:LANES * tile + LANES]

    def adapters(layer, reorder=False):
        for c in range(0, FF, HIDDEN):
            blocks = stack_right(rows8(adapt_b[layer, :, c:c + HIDDEN]))
            if reorder:
                moved = dot(jnp.concatenate([*blocks[:3], blocks[0]], axis=0).astype(BF16), perm[...])
                for tile in range(NT):
                    o = slice(LANES * tile, LANES * tile + LANES)
                    hi, mid, lo = moved[0:8, o], moved[8:16, o], moved[16:24, o]
                    first = UP_TILE * tile + c // HIDDEN * LANES
                    write_blocks(b6.at[:, first:first + LANES], (hi, mid, lo, hi, mid, hi))
            else:
                write_blocks(b6.at[:, c:c + HIDDEN], blocks)
        write_blocks(a6, stack_right(rows8(adapt_a[layer])))

    def normalize(layer, save):
        @pl.loop(0, TOKENS // LANES)
        def _(i):
            r = pl.ds(pl.multiple_of(i * LANES, LANES), LANES)
            xf = x[r, :].astype(F32)
            inv = lax.rsqrt(jnp.mean(xf * xf, axis=-1, keepdims=True) + NORM_EPS)
            u[r, :] = (xf * inv).astype(BF16)
            inv_s[layer, r, :] = jnp.broadcast_to(inv, (LANES, LANES))

        if layer < LAYERS - 1:
            adapters(layer)
        low = sum3(dot_t(a6[0:32, :], u[...]))
        left = stack_left(low)
        v3[layer, :, :] = jnp.concatenate([left[0], left[3], left[5]], axis=0)
        wide = jnp.concatenate(list(left) + [jnp.zeros((80, TOKENS), F32)], axis=0)
        v6[...] = jnp.transpose(wide).astype(BF16)
        if save:
            save_x(layer).start()
            save_u(layer).start()

    def save_x(layer):
        return pltpu.make_async_copy(x, resids.at[layer], load_sem.at[4])

    def save_u(layer):
        return pltpu.make_async_copy(u, normeds.at[layer], load_sem.at[5])

    def first_load(layer, t, buf):
        return pltpu.make_async_copy(land_up.at[lax.rem(layer, 2), :, pl.ds(pl.multiple_of(UP_TILE * t, LANES), UP_TILE)], buf.at[lax.rem(t, 2)], w_sem.at[0, lax.rem(t, 2)])

    def act_store(layer, t, acts):
        return pltpu.make_async_copy(acts.at[lax.rem(t, 2)], slopes.at[layer, :, pl.ds(pl.multiple_of(UP_TILE * t, LANES), UP_TILE)], act_sem.at[lax.rem(t, 2)])

    def keep_half(layer, t, h, buf):
        block = 2 * t + h - 5 * quarter
        copy = pltpu.make_async_copy(buf.at[lax.rem(t, 2), :, 256 * h:256 * h + 256],
                                     back_up.at[layer, 0, :, pl.ds(pl.multiple_of(256 * jnp.clip(block, 0, 4), LANES), 256)], keep_sem.at[h])
        return jnp.logical_and(block >= 0, block < 5), copy

    def first_product(layer, t, buf, acts, s):
        first_load(layer, t, buf).wait()
        for h in range(2):
            cond, copy = keep_half(layer, t, h, buf)
            pl.when(cond)(copy.start)

        @pl.when(t >= 2)
        def _():
            act_store(layer, t - 2, acts).wait()

        c = pl.ds(pl.multiple_of(UP_TILE * t, LANES), UP_TILE)
        pre = dot(u[...], buf[lax.rem(t, 2)]) + dot(v6[...], b6[:, c])
        act = pre.astype(BF16)
        hidden, slope = gelu_both(act)
        s[:, c] = hidden.astype(BF16)
        acts[lax.rem(t, 2)] = slope
        act_store(layer, t, acts).start()
        for h in range(2):
            cond, copy = keep_half(layer, t, h, buf)
            pl.when(cond)(copy.wait)

    def second_load(layer, c, buf):
        return pltpu.make_async_copy(land_down.at[lax.rem(layer, 2), :, pl.ds(pl.multiple_of(OUT_COLS * c, LANES), OUT_COLS)], buf.at[lax.rem(c, 2)], w_sem.at[1, lax.rem(c, 2)])

    def second_keep(layer, c, buf):
        cc = pl.ds(pl.multiple_of(OUT_COLS * c, LANES), OUT_COLS)
        return pltpu.make_async_copy(buf.at[lax.rem(c, 2), pl.ds(pl.multiple_of(QUARTER * quarter, 16), QUARTER), :], back_down.at[layer, 0, :, cc], keep_sem.at[2])

    def second_product(layer, c, buf, s):
        second_load(layer, c, buf).wait()
        keep = second_keep(layer, c, buf)
        keep.start()
        cc = pl.ds(pl.multiple_of(OUT_COLS * c, LANES), OUT_COLS)
        x[:, cc] = (x[:, cc].astype(F32) + dot(s[...], buf[lax.rem(c, 2)])).astype(BF16)
        keep.wait()

    def gelu_both(act):
        af = act.astype(F32)
        x2, th = gelu_inner(af)
        half = 0.5 * af
        slope = 0.5 + 0.5 * th + half * (1.0 - th * th) * (GELU_S + (3.0 * GELU_S * GELU_C) * x2)
        return half + half * th, slope

    def low_parts(layer, dpre, *places):
        width = dpre.shape[1] // len(places)
        dlow[...] += sum3(dot_t(jnp.concatenate([b6[0:32, pl.ds(c, width)] for c in places], axis=1), dpre))
        share = sum3(dot(v3[layer].astype(BF16), dpre))
        for i, c in enumerate(places):
            gb[:, pl.ds(c, width)] = share[:, width * i:width * i + width]

    def natural_order():
        for m in range(FF // HIDDEN):
            piece = jnp.concatenate([grad_b[LAYERS - 1, :, UP_TILE * tile + LANES * m:UP_TILE * tile + LANES * m + LANES] for tile in range(NT)], axis=1)
            parts = jnp.concatenate(split3(rows8(piece)), axis=0).astype(BF16)
            gb[:, HIDDEN * m:HIDDEN * m + HIDDEN] = sum3(dot_t(parts, perm[...]))
        grad_b[LAYERS - 1, :, :] = gb[0:RANK, :]

    def close_layer(layer, acc):
        left = stack_left(dlow[...])
        wide = jnp.concatenate(list(left) + [jnp.zeros((80, TOKENS), F32)], axis=0)
        v6[...] = jnp.transpose(wide).astype(BF16)
        narrow = jnp.concatenate([left[0], left[3], left[5]], axis=0).astype(BF16)
        ga = sum3(dot(narrow, u[...]))
        send_g[layer, 0:RANK, 0:G_EDGE] = gb[0:RANK, 0:G_EDGE]
        send_g[layer, RANK:2 * RANK, 0:FF - G_EDGE] = gb[0:RANK, G_EDGE:FF]
        send_g[layer, RANK:2 * RANK, FF - G_EDGE:G_EDGE] = ga[0:RANK]
        send_g[layer, :, G_EDGE:G_COLS] = jnp.zeros((8, G_COLS - G_EDGE), F32)
        g_step(layer, 0)

        @pl.loop(0, TOKENS // OUT_COLS)
        def _(i):
            r = pl.ds(pl.multiple_of(i * OUT_COLS, OUT_COLS), OUT_COLS)
            pl.when(jnp.logical_and(layer == 0, i == 1))(lambda: g_step(0, 1))
            side = dot(v6[r, :], a6[...]).astype(BF16)
            dn = (acc[r, :].astype(BF16) + side).astype(F32)
            xf = x[r, :].astype(F32)
            inv = inv_s[layer, r, 0:1]
            row = jnp.mean(xf * dn, axis=-1, keepdims=True)
            d[r, :] = (d[r, :].astype(F32) + inv * dn - xf * (inv * inv * inv * row)).astype(BF16)

    zero128 = jnp.zeros((80, HIDDEN), BF16)
    a6[48:LANES, :] = zero128
    for c in range(0, FF, HIDDEN):
        b6[48:LANES, c:c + HIDDEN] = zero128

    def forward(buf_a, buf_b, s, acts):
        def iteration(j, carry):
            i = j - LEAD

            pl.when(i == MIX - FAR_LEAD)(wait_credits)
            gather_step(i)

            @pl.when(i == -2)
            def _():
                loads[2].wait()
                normalize(0, True)

            second = i >= 2 * NT + 4
            layer = jnp.where(second, 1, 0)
            lo = jnp.where(second, 2 * NT + 5, 1)

            @pl.when(jnp.logical_and(i >= lo - 1, i < lo - 1 + NT))
            def _():
                first_load(layer, i - lo + 1, buf_a).start()

            @pl.when(jnp.logical_and(i >= lo, i < lo + NT))
            def _():
                first_product(layer, i - lo, buf_a, acts, s)

            @pl.when(i == lo + NT)
            def _():
                act_store(layer, NT - 2, acts).wait()
                act_store(layer, NT - 1, acts).wait()

            pl.when(i == NT + 2)(build_order)
            pl.when(i == MIX - 3)(lambda: adapters(LAYERS - 1, reorder=True))
            pieces = HIDDEN // OUT_COLS
            prev = jnp.where(i >= 4 * NT - 1, 1, 0)
            lo2 = 2 * NT + 2 * NT * prev

            @pl.when(jnp.logical_and(i >= lo2 - 1, i < lo2 - 1 + pieces))
            def _():
                second_load(prev, i - lo2 + 1, buf_b).start()

            @pl.when(i == lo2)
            def _():
                save_x(prev).wait()
                save_u(prev).wait()

            @pl.when(jnp.logical_and(i >= lo2, i < lo2 + pieces))
            def _():
                second_product(prev, i - lo2, buf_b, s)

            @pl.when(i == 2 * NT + pieces - 1)
            def _():
                give_credits()
                normalize(1, True)

            @pl.when(i == 4 * NT + pieces - 1)
            def _():
                normalize(2, False)
            return carry

        lax.fori_loop(0, FUSED_FROM + LEAD, iteration, 0)

    pl.run_scoped(
        forward,
        pltpu.VMEM((2, HIDDEN, UP_TILE), BF16), pltpu.VMEM((2, FF, OUT_COLS), BF16),
        pltpu.VMEM((TOKENS, FF), BF16), pltpu.VMEM((2, TOKENS, UP_TILE), F32),
    )

    loads[3].wait()

    last = LAYERS - 1

    def fused_loads(t, buf_a, buf_b):
        rows = land_down.reshape(2, 32, DOWN_ROWS, HIDDEN).at[last % 2, :, pl.ds(pl.multiple_of(DOWN_TILE * t, 16), DOWN_TILE), :]
        return first_load(last, t, buf_a), pltpu.make_async_copy(rows, buf_b.at[lax.rem(t, 2)], w_sem.at[1, lax.rem(t, 2)])

    def fused(buf_a, buf_b, dpre, y, acc, out):
        y[...] = jnp.zeros_like(y)
        acc[...] = jnp.zeros_like(acc)
        dlow[...] = jnp.zeros_like(dlow)
        for matrix in range(2):
            swap_own(LAYERS - 2, matrix).start()

        for load in fused_loads(0, buf_a, buf_b):
            load.start()

        def iteration(i, carry):
            gather_step(i)
            early, ticks = i - BACK_FROM, lax.rem(i - BACK_FROM, BACK_EVERY)
            pl.when(jnp.logical_and(jnp.logical_and(early >= 0, i < BACK_STEADY), ticks == 0))(lambda: send_back(early // BACK_EVERY))
            pl.when(i >= BACK_STEADY)(lambda: send_back(BACK_EARLY + i - BACK_STEADY))

            catch_up = i < FUSED_FROM + 2
            t_load = jnp.where(i == FUSED_FROM, 1, (i - MIX - 2) // 2)

            @pl.when(jnp.logical_and(jnp.logical_or(i == FUSED_FROM, lax.rem(i, 2) == 0), t_load < NT))
            def _():
                for load in fused_loads(t_load, buf_a, buf_b):
                    load.start()

            first_half = jnp.where(catch_up, 2 * (i - FUSED_FROM), i - FUSED_FROM + 2)

            @pl.loop(first_half, jnp.where(catch_up, first_half + 2, first_half + 1))
            def _(g):
                t, h = g // 2, lax.rem(g, 2)
                slot = lax.rem(t, 2)

                @pl.when(h == 0)
                def _():
                    for load in fused_loads(t, buf_a, buf_b):
                        load.wait()

                c = pl.multiple_of(UP_TILE * t, LANES)
                r = pl.ds(pl.multiple_of(ROWS * h, ROWS), ROWS)
                down = buf_b.at[slot]
                pre = dot(u[r, :], buf_a[slot]) + dot(v6[r, :], b6[:, pl.ds(c, UP_TILE)])
                dh = dot_t(d[r, :], down[...].reshape(UP_TILE, HIDDEN)).astype(BF16).astype(F32)
                s, slope = gelu_both(pre.astype(BF16))
                dp = (dh * slope).astype(BF16)
                dpre[r, :] = dp
                y[r, :] += dot(s.astype(BF16), down[...].reshape(UP_TILE, HIDDEN))
                acc[r, :] += dot_t(dp, buf_a[slot])

                @pl.when(h == 1)
                def _():
                    low_parts(last, dpre[...], c)
            return carry

        lax.fori_loop(FUSED_FROM, FUSED_TO, iteration, 0)

        pl.loop(BACK_SENT, BACK_SENT + BACK_AHEAD)(send_back)

        @pl.loop(0, TOKENS // LANES)
        def _(i):
            r = pl.ds(pl.multiple_of(i * LANES, LANES), LANES)
            out[r, :] = (x[r, :].astype(F32) + y[r, :]).astype(BF16)

        out_copy = pltpu.make_async_copy(out, out_tokens, load_sem.at[6])
        out_copy.start()
        close_layer(last, acc)
        out_copy.wait()

    pl.run_scoped(
        fused,
        pltpu.VMEM((2, HIDDEN, UP_TILE), BF16), pltpu.VMEM((2, 32, DOWN_TILE, HIDDEN), BF16), pltpu.VMEM((TOKENS, UP_TILE), BF16),
        pltpu.VMEM((TOKENS, HIDDEN), F32), pltpu.VMEM((TOKENS, HIDDEN), F32), pltpu.VMEM((TOKENS, HIDDEN), BF16),
    )

    steps = 2 * SUBS

    def backward(buf_a, buf_b, act, dpre, acc):
        def place(n):
            layer, b = (LAYERS - 2) - n // steps, lax.rem(n, steps)
            outside, sub = b // SUBS, lax.rem(b, SUBS)
            base = 2 * (parity + outside - 2 * parity * outside)
            return layer, b, outside, sub, [pl.multiple_of(QUARTER * (base + c) + SUB * sub, SUB) for c in (core, 1 - core)]

        def loads_of(n):
            layer, _, outside, sub, fs = place(n)
            s = lax.rem(n, 2)
            copies = []
            for i in range(2):
                half = pl.ds(SUB * i, SUB)
                copies += [(back_ref(0, layer, 2 * outside + i, sub), buf_a.at[s, :, half]), (back_ref(1, layer, 2 * outside + i, sub), buf_b.at[s, half, :]),
                           (slopes.at[layer, :, pl.ds(fs[i], SUB)], act.at[s, :, half])]
            return [pltpu.make_async_copy(src, dst, back_sem.at[s, i]) for i, (src, dst) in enumerate(copies)]

        def pass_on(n):
            layer, _, outside, sub, _ = place(n)

            @pl.when(jnp.logical_and(n < 2 * steps, outside == 1))
            def _():
                for matrix in range(2):
                    for axis in range(3):
                        back_copy(matrix, layer, sub, axis).wait_recv()
                    swap_sub(matrix, layer, sub).start()

        def fetch(n):
            layer, b, outside, sub, _ = place(n)

            @pl.when(b == 0)
            def _():
                for matrix in range(2):
                    swap_own(layer, matrix).wait_recv()

            @pl.when(outside == 1)
            def _():
                for matrix in range(2):
                    swap_sub(matrix, layer, sub).wait_recv()

            for load in loads_of(n):
                load.start()

        def reloads(layer):
            return (pltpu.make_async_copy(resids.at[layer], x, load_sem.at[4]), pltpu.make_async_copy(normeds.at[layer], u, load_sem.at[5]))

        for matrix in range(2):
            swap_own(0, matrix).start()
        fetch(0)

        def iteration(n, carry):
            layer, b, _, _, fs = place(n)
            s = lax.rem(n, 2)

            @pl.when(b == 0)
            def _():
                for load in reloads(layer):
                    load.start()
                adapters(layer)
                acc[...] = jnp.zeros_like(acc)
                dlow[...] = jnp.zeros_like(dlow)

            h = n + BACK_SENT + BACK_AHEAD
            pl.when(h < 4 * SUBS)(lambda: send_back(h))
            for stage in range(1, G_STAGES + 1):
                for done in range(1, LAYERS):
                    pl.when(n == SUMS_FROM + stage - done)(lambda: g_step(done, stage))
            for load in loads_of(n):
                load.wait()
            pass_on(n + 2)
            pl.when(n + 1 < 2 * steps)(lambda: fetch(n + 1))
            for h in range(TOKENS // ROWS):
                r = slice(ROWS * h, ROWS * h + ROWS)
                dh = dot_t(d[r, :], buf_b[s]).astype(BF16).astype(F32)
                dp = (dh * act[s, r, :]).astype(BF16)
                dpre[r, :] = dp
                acc[r, :] += dot_t(dp, buf_a[s])
            low_parts(layer, dpre[...], *fs)

            @pl.when(b == steps - 1)
            def _():
                for load in reloads(layer):
                    load.wait()
                close_layer(layer, acc)
            return carry

        lax.fori_loop(0, 2 * steps, iteration, 0)
        grad_copy = pltpu.make_async_copy(d, grad_tokens, load_sem.at[6])
        grad_copy.start()
        g_step(0, 2)
        pl.loop(1, LAYERS)(g_finish)
        natural_order()
        for stage in range(3, G_STAGES + 1):
            g_step(0, stage)
        g_finish(0)
        grad_copy.wait()

    pl.run_scoped(
        backward,
        pltpu.VMEM((2, HIDDEN, 2 * SUB), BF16), pltpu.VMEM((2, 2 * SUB, HIDDEN), BF16), pltpu.VMEM((2, TOKENS, 2 * SUB), F32),
        pltpu.VMEM((TOKENS, 2 * SUB), BF16), pltpu.VMEM((TOKENS, HIDDEN), F32),
    )

    @pl.loop(0, LAYERS - 1)
    def _(layer):
        for matrix in range(2):
            swap_own(layer, matrix).wait_send()

            @pl.loop(0, SUBS)
            def _(sub):
                swap_sub(matrix, layer, sub).wait_send()
                for axis in range(3):
                    back_copy(matrix, layer, sub, axis).wait_send()


def step(tokens, cotangent, w_up, w_down, adapt_a, adapt_b):
    any_spec, vmem = pl.BlockSpec(memory_space=pl.ANY), pl.BlockSpec(memory_space=pltpu.VMEM)
    sds = jax.ShapeDtypeStruct
    dma = pltpu.SemaphoreType.DMA
    outs = [
        (sds((TOKENS, HIDDEN), BF16), any_spec), (sds((TOKENS, HIDDEN), BF16), any_spec),
        (sds((LAYERS, RANK, HIDDEN), F32), vmem), (sds((LAYERS, RANK, FF), F32), vmem),
        (sds((2, HIDDEN, FF), BF16), any_spec), (sds((2, FF, HIDDEN), BF16), any_spec),
        (sds((2, 4, HIDDEN, QUARTER), BF16), any_spec), (sds((2, 4, QUARTER, HIDDEN), BF16), any_spec),
        (sds((2, TOKENS, FF), F32), any_spec), (sds((2, TOKENS, HIDDEN), BF16), any_spec), (sds((2, TOKENS, HIDDEN), BF16), any_spec),
    ]
    result = pl.pallas_call(
        step_kernel,
        out_shape=[o[0] for o in outs],
        in_specs=[any_spec] * 4 + [vmem] * 2,
        out_specs=[o[1] for o in outs],
        scratch_shapes=[
            pltpu.VMEM((LAYERS, UP_ROWS, FF), BF16), pltpu.VMEM((LAYERS, DOWN_ROWS, HIDDEN), BF16),
            pltpu.VMEM((TOKENS, HIDDEN), BF16), pltpu.VMEM((TOKENS, HIDDEN), BF16), pltpu.VMEM((TOKENS, HIDDEN), BF16),
            pltpu.VMEM((LAYERS, TOKENS, LANES), F32), pltpu.VMEM((LANES, FF), BF16), pltpu.VMEM((LANES, HIDDEN), BF16),
            pltpu.VMEM((TOKENS, LANES), BF16), pltpu.VMEM((LAYERS, 24, TOKENS), F32), pltpu.VMEM((HIDDEN, HIDDEN), BF16), pltpu.VMEM((8, TOKENS), F32), pltpu.VMEM((8, FF), F32),
            pltpu.VMEM((LAYERS, 8, G_COLS), F32), pltpu.VMEM((LAYERS, 5, 8, G_HALF), F32), pltpu.VMEM((LAYERS, 8, G_HALF), F32),
            pltpu.VMEM((LAYERS, 4, 8, G_HALF), F32), pltpu.VMEM((LAYERS, 8, G_HALF), F32),
            dma((RING, 16)), dma((RING, 4)), dma((SRING, 22)), dma((2, 2, SUBS, 3)), dma((2, 2, SUBS, 3)), dma((2, 2, SUBS + 1)), dma((2, 2, SUBS + 1)),
            dma((LAYERS, G_STAGES)), dma((LAYERS, G_STAGES)), dma((7,)), dma((2, 6)), dma((2, 2)), dma((2,)), dma((3,)), pltpu.SemaphoreType.REGULAR,
        ],
        compiler_params=pltpu.CompilerParams(collective_id=0, has_side_effects=True, vmem_limit_bytes=67_000_000),
        cost_estimate=pl.CostEstimate(flops=12 * 2 * TOKENS * HIDDEN * FF, bytes_accessed=400_000_000, transcendentals=0),
        name="mlp_stack",
    )(tokens, cotangent, w_up, w_down, jnp.swapaxes(adapt_a, 1, 2), adapt_b)
    return result[0], result[1], jnp.swapaxes(result[2], 1, 2), result[3]


def solution(mesh):
    tok_spec, weight_spec = P(GROUP, None), P(None, GROUP, None)
    return jax.shard_map(step, mesh=mesh, in_specs=(tok_spec, tok_spec, weight_spec, weight_spec, P(), P()), out_specs=(tok_spec, tok_spec, P(), P()), check_vma=False)
```

```python
import math

import jax
import jax.numpy as jnp
from jax import lax
from jax.experimental import pallas as pl
from jax.experimental.pallas import tpu as pltpu
from jax.sharding import PartitionSpec as P

GROUP = ("data", "local")
MESH = pl.DeviceIdType.MESH
BF16, F32 = jnp.bfloat16, jnp.float32
ROWS = 512
LANES = 128
NORM_EPS = 1e-6
GELU_S = math.sqrt(2.0 / math.pi)
GELU_C = 0.044715

LAYERS, TOKENS, HIDDEN, FF, RANK = 3, 1024, 1280, 5120, 4
NT = 10
TILES = 2 * LAYERS * NT
UP_ROWS, DOWN_ROWS = HIDDEN // 32, FF // 32
UP_TILE, DOWN_TILE = FF // NT, DOWN_ROWS // NT
OUT_COLS = 256
QUARTER = FF // 4
RING, SRING = 28, 16
OFFSETS = (7, 6, 5, 4, 3, 2, 1, 0, -1)
LEAD = OFFSETS[0]
FAR_LEAD = 2 * LEAD - 1
MIX = 4 * NT
FUSED_FROM = MIX + HIDDEN // OUT_COLS
FUSED_TO = FUSED_FROM + 2 * NT - 2
BACK_FROM = 48
BACK_EARLY, BACK_EVERY = 3, 3
BACK_STEADY = BACK_FROM + BACK_EVERY * BACK_EARLY - 1
BACK_SENT = BACK_EARLY + FUSED_TO - BACK_STEADY
BACK_AHEAD = 2
SUMS_FROM = 14
SUB = 256
SUBS = QUARTER // SUB
G_COLS = 3328
G_HALF = G_COLS // 2
G_EDGE = (FF + HIDDEN) // 2
G_STAGES = 6
SPLITS = (((0, 424), (424, 424), (848, 432)), ((0, 88), (88, 88), (176, 80)))


def dot(a, b):
    return jnp.dot(a, b, preferred_element_type=F32)


def dot_t(a, b):
    return lax.dot_general(a, b, (((1,), (1,)), ((), ())), preferred_element_type=F32)


def split3(x):
    hi = x.astype(BF16).astype(F32)
    rest = x - hi
    mid = rest.astype(BF16).astype(F32)
    return hi, mid, (rest - mid).astype(BF16).astype(F32)


def stack_left(x):
    hi, mid, lo = split3(x)
    return hi, hi, hi, mid, mid, lo


def stack_right(x):
    hi, mid, lo = split3(x)
    return hi, mid, lo, hi, mid, hi


def sum3(x):
    return x[0:8] + x[8:16] + x[16:24]


def gelu_inner(x):
    x2 = x * x
    return x2, jnp.tanh(x * (GELU_S + (GELU_S * GELU_C) * x2))


def step_kernel(
    tokens, cotangent, w_up, w_down, adapt_a, adapt_b,
    out_tokens, grad_tokens, grad_a, grad_b,
    land_up, land_down, back_up, back_down, slopes, resids, normeds,
    own_up, own_down, x, u, d, inv_s, b6, a6, v6, v3, perm, dlow, gb, send_g, half_g, recv_first, recv_half, recv_last,
    recv_sem, pair_sem, send_sem, back_recv, back_send, swap_recv, swap_send, g_recv, g_send, load_sem, back_sem, w_sem, act_sem, keep_sem, credit,
):
    z = lax.axis_index("local")
    dev = lax.axis_index("data")
    core = lax.rem(dev, 2)
    dx = dev + 2 - 4 * lax.rem(dev // 2, 2)
    dy = dev + 4 - 8 * (dev // 4)
    dd = dx + dy - dev
    dc = dev + 1 - 2 * core
    zp = z + 1 - 2 * lax.rem(z, 2)
    za, zb = 3 - z, 3 - zp
    parity = lax.rem(lax.rem(dev // 2, 2) + dev // 4 + z, 2)
    is_end = jnp.logical_or(z == 0, z == 3)
    is_mid = jnp.logical_not(is_end)
    to_p, to_a, to_b = (zp, dev), (za, dev), (zb, dev)
    to_x, to_y, to_c = (z, dx), (z, dy), (z, dc)
    cols = (dev, dx, dy, dd)
    pair_cols = (dc, dc + dx - dev, dc + dy - dev, dc + dd - dev)

    def remote(src, dst, ssem, rsem, target):
        return pltpu.make_async_remote_copy(src, dst, ssem, rsem, device_id=target, device_id_type=MESH)

    def both(cond, on, off):
        pl.when(cond)(on)
        pl.when(jnp.logical_not(cond))(off)

    loads = [
        pltpu.make_async_copy(w_up, own_up, load_sem.at[0]),
        pltpu.make_async_copy(w_down, own_down, load_sem.at[1]),
        pltpu.make_async_copy(tokens, x, load_sem.at[2]),
        pltpu.make_async_copy(cotangent, d, load_sem.at[3]),
    ]
    for load in loads:
        load.start()
    barrier = pltpu.get_barrier_semaphore()
    for target in (to_p, to_x, to_y, to_c, to_b):
        pl.semaphore_signal(barrier, inc=1, device_id=target, device_id_type=MESH)

    @pl.when(is_mid)
    def _():
        pl.semaphore_signal(barrier, inc=1, device_id=to_a, device_id_type=MESH)
        pl.semaphore_wait(barrier, 6)

    @pl.when(is_end)
    def _():
        pl.semaphore_wait(barrier, 5)

    loads[0].wait()
    loads[1].wait()

    def is_up(k):
        return jnp.where(k < MIX, lax.rem(k // NT, 2) == 0, lax.rem(k, 2) == 1)

    def tile_of(k):
        return jnp.where(k < MIX, lax.rem(k, NT), (k - MIX) // 2)

    def slab(up, k, col, zz, own=False):
        layer, t, n = k // (2 * NT), tile_of(k), 4 * col + zz
        slot = lax.rem(layer, 2)
        if up:
            c = pl.ds(pl.multiple_of(UP_TILE * t, LANES), UP_TILE)
            return own_up.at[layer, :, c] if own else land_up.at[slot, pl.ds(pl.multiple_of(UP_ROWS * n, 8), UP_ROWS), c]
        r = pl.multiple_of(DOWN_TILE * t, 16)
        return own_down.at[layer, pl.ds(r, DOWN_TILE), :] if own else land_down.at[slot, pl.ds(pl.multiple_of(DOWN_ROWS * n + r, 16), DOWN_TILE), :]

    def send(up, k, entry):
        rel, zz, target, to_rel = entry
        own = rel == own_c and zz is z
        index = [e is entry for e in order].index(True)
        return remote(slab(up, k, cols[rel], zz, own), slab(up, k, cols[rel], zz), send_sem.at[lax.rem(k, SRING), index],
                      recv_sem.at[lax.rem(k, RING), to_rel * 4 + zz], target)

    def wait_slab(up, k, rel, zz):
        s = slab(up, k, cols[rel], zz)
        remote(s, s, send_sem.at[0, 0], recv_sem.at[lax.rem(k, RING), rel * 4 + zz], to_x).wait_recv()

    def pair_copy(up, k, g, c):
        layer, t = k // (2 * NT), tile_of(k)
        slot = lax.rem(layer, 2)
        if up:
            s = land_up.at[slot, pl.ds(pl.multiple_of(4 * UP_ROWS * c, 8), 4 * UP_ROWS), pl.ds(pl.multiple_of(UP_TILE * t, LANES), UP_TILE)]
        else:
            s = land_down.reshape(2, 32, DOWN_ROWS, HIDDEN).at[slot, pl.ds(4 * c, 4), pl.ds(pl.multiple_of(DOWN_TILE * t, 16), DOWN_TILE), :]
        return remote(s, s, send_sem.at[lax.rem(k, SRING), len(order) + 1 + g], pair_sem.at[lax.rem(k, RING), g], to_c)

    own_c, x_c, y_c, diag_c = range(4)
    own_sends = [(own_c, z, to_p, own_c), (own_c, z, to_a, own_c), (own_c, z, to_x, x_c), (own_c, z, to_y, y_c)]
    hop_p = [(own_c, zp, to_x, x_c), (own_c, zp, to_y, y_c), (own_c, zp, to_a, own_c)]
    hop_a = [(own_c, za, to_p, own_c), (own_c, za, to_x, x_c), (own_c, za, to_y, y_c)]
    hop_b = [(own_c, zb, to_p, own_c), (own_c, zb, to_x, x_c), (own_c, zb, to_y, y_c)]
    diag = [(y_c, z, to_x, diag_c), (x_c, zb, to_y, diag_c)]
    swap = [(diag_c, z, to_p, diag_c), (diag_c, zb, to_p, diag_c)]
    order = own_sends + hop_p + hop_a + hop_b + diag + swap

    def each(up, k, entries, act):
        for entry in entries:
            rel, zz, target, _ = entry
            if target is to_a or (target is to_p and rel == own_c and zz is not z):
                @pl.when(is_mid)
                def _():
                    act(send(up, k, entry))
            else:
                act(send(up, k, entry))

    def start(up, k, entries):
        each(up, k, entries, lambda copy: copy.start())

    def own_local(up, k):
        return pltpu.make_async_copy(slab(up, k, dev, z, True), slab(up, k, dev, z), send_sem.at[lax.rem(k, SRING), len(order)])

    def stage_own(up, k):
        start(up, k, own_sends)
        own_local(up, k).start()

    def stage_1(up, k):
        wait_slab(up, k, own_c, zp)
        start(up, k, hop_p)

        @pl.when(is_mid)
        def _():
            wait_slab(up, k, own_c, za)
            start(up, k, hop_a)

    def stage_2(up, k):
        wait_slab(up, k, own_c, zb)
        start(up, k, hop_b)

    def stage_3(up, k):
        @pl.when(is_end)
        def _():
            wait_slab(up, k, own_c, za)
            start(up, k, hop_a[1:])

    def stage_diag(up, k):
        wait_slab(up, k, y_c, z)
        start(up, k, diag[:1])
        wait_slab(up, k, x_c, zb)
        start(up, k, diag[1:])

    def stage_swap(up, k):
        wait_slab(up, k, diag_c, z)
        start(up, k, swap[:1])
        wait_slab(up, k, diag_c, zb)
        start(up, k, swap[1:])

    def stage_pair(up, k):
        own_local(up, k).wait()
        pair_copy(up, k, own_c, dev).start()
        for zz in (z, zp, za):
            wait_slab(up, k, x_c, zz)
        pair_copy(up, k, x_c, dx).start()
        for zz in (zp, za, zb):
            wait_slab(up, k, y_c, zz)
        pair_copy(up, k, y_c, dy).start()
        for zz in (zp, za):
            wait_slab(up, k, diag_c, zz)
        pair_copy(up, k, diag_c, dd).start()

    def stage_done(up, k):
        for g in range(4):
            pair_copy(up, k, g, pair_cols[g]).wait_recv()

    def stage_sent(up, k):
        each(up, k, order, lambda copy: copy.wait_send())
        for g in range(4):
            pair_copy(up, k, g, cols[g]).wait_send()

    stages = list(zip(OFFSETS[:0:-1], (stage_sent, stage_done, stage_pair, stage_swap, stage_diag, stage_3, stage_2, stage_1)))

    def at_tile(k, stage):
        @pl.when(jnp.logical_and(k >= 0, k < TILES))
        def _():
            both(is_up(k), lambda: stage(True, k), lambda: stage(False, k))

    def gather_step(i):
        for offset, stage in stages:
            at_tile(i + offset, stage)
        first = jnp.minimum(2 * (i + LEAD), i + FAR_LEAD)

        @pl.loop(first, jnp.minimum(2 * (i + LEAD) + 2, i + FAR_LEAD + 1))
        def _(k):
            at_tile(k, stage_own)

    def give_credits():
        for target in (to_p, to_x, to_y, to_c):
            pl.semaphore_signal(credit, inc=1, device_id=target, device_id_type=MESH)

        @pl.when(is_mid)
        def _():
            pl.semaphore_signal(credit, inc=1, device_id=to_a, device_id_type=MESH)

    def wait_credits():
        @pl.when(is_mid)
        def _():
            pl.semaphore_wait(credit, 5)

        @pl.when(is_end)
        def _():
            pl.semaphore_wait(credit, 4)

    quarter = 2 * parity + core

    def back_ref(matrix, layer, slot, sub, part=None):
        c = pl.ds(pl.multiple_of(SUB * sub, SUB), SUB)
        if matrix == 0:
            return back_up.at[layer, slot, :, c] if part is None else back_up.at[layer, slot, pl.ds(*part), c]
        if part is None:
            return back_down.at[layer, slot, c, :]
        return back_down.at[layer, slot, pl.ds(pl.multiple_of(SUB * sub + part[0], 8), part[1]), :]

    def back_copy(matrix, layer, sub, axis):
        part = SPLITS[matrix][axis]
        return remote(back_ref(matrix, layer, 0, sub, part), back_ref(matrix, layer, 2, sub, part), back_send.at[matrix, layer, sub, axis],
                      back_recv.at[matrix, layer, sub, axis], (to_x, to_y, to_p)[axis])

    def send_back(h):
        layer, sub = (LAYERS - 2) - h // (2 * SUBS), lax.rem(h, 2 * SUBS) // 2
        for matrix in range(2):
            @pl.when(lax.rem(h, 2) == matrix)
            def _():
                for axis in range(3):
                    back_copy(matrix, layer, sub, axis).start()

    def swap_own(layer, matrix):
        ref = (back_up, back_down)[matrix]
        return remote(ref.at[layer, 0], ref.at[layer, 1], swap_send.at[matrix, layer, SUBS], swap_recv.at[matrix, layer, SUBS], to_c)

    def swap_sub(matrix, layer, sub):
        return remote(back_ref(matrix, layer, 2, sub), back_ref(matrix, layer, 3, sub), swap_send.at[matrix, layer, sub], swap_recv.at[matrix, layer, sub], to_c)

    def g_copy(layer, stage):
        half = lambda c: pl.ds(pl.multiple_of(G_HALF * c, LANES), G_HALF)
        if stage == 0:
            src, dst, target = send_g.at[layer, :, half(1 - core)], recv_first.at[layer], to_c
        elif stage == 5:
            src, dst, target = half_g.at[layer, 4], recv_last.at[layer], to_c
        else:
            src, dst, target = half_g.at[layer, stage - 1], recv_half.at[layer, stage - 1], (to_x, to_y, to_p, to_b)[stage - 1]
        return remote(src, dst, g_send.at[layer, stage], g_recv.at[layer, stage], target)

    def g_step(layer, stage):
        if stage > 0:
            g_copy(layer, stage - 1).wait()
        if stage == 1:
            half_g[layer, 0] = send_g[layer, :, pl.ds(pl.multiple_of(G_HALF * core, LANES), G_HALF)] + recv_first[layer]
        elif 1 < stage < 6:
            half_g[layer, stage - 1] = half_g[layer, stage - 2] + recv_half[layer, stage - 2]
        if stage < 6:
            g_copy(layer, stage).start()

    def g_finish(layer):
        send_g[layer, :, pl.ds(pl.multiple_of(G_HALF * core, LANES), G_HALF)] = half_g[layer, 4]
        send_g[layer, :, pl.ds(pl.multiple_of(G_HALF * (1 - core), LANES), G_HALF)] = recv_last[layer]
        total = send_g[layer]
        grad_b[layer, :, 0:G_EDGE] = total[0:RANK, 0:G_EDGE]
        grad_b[layer, :, G_EDGE:FF] = total[RANK:2 * RANK, 0:FF - G_EDGE]
        grad_a[layer, :, :] = total[RANK:2 * RANK, FF - G_EDGE:G_EDGE]

    def write_blocks(ref, blocks):
        for i in range(3):
            ref[16 * i:16 * i + 16, :] = jnp.concatenate([blocks[2 * i], blocks[2 * i + 1]], axis=0).astype(BF16)

    def rows8(value):
        return jnp.concatenate([value, jnp.zeros_like(value)], axis=0)

    def build_order():
        @pl.loop(0, HIDDEN // OUT_COLS)
        def _(block):
            o = lax.broadcasted_iota(jnp.int32, (HIDDEN, OUT_COLS), 1) + OUT_COLS * block
            c = lax.broadcasted_iota(jnp.int32, (HIDDEN, OUT_COLS), 0)
            tile, place = o // LANES, o % LANES
            source = DOWN_ROWS * (place // DOWN_TILE) + DOWN_TILE * tile + place % DOWN_TILE
            perm[:, pl.ds(pl.multiple_of(OUT_COLS * block, OUT_COLS), OUT_COLS)] = jnp.where(c == source, 1.0, 0.0).astype(BF16)

        parts = FF // HIDDEN
        moved = [dot(own_up[LAYERS - 1, :, HIDDEN * m:HIDDEN * m + HIDDEN], perm[:]).astype(BF16) for m in range(parts)]
        for m in range(parts):
            for tile in range(NT):
                first = UP_TILE * tile + LANES * m
                own_up[LAYERS - 1, :, first:first + LANES] = moved[m][:, LANES * tile:LANES * tile + LANES]

    def adapters(layer, reorder=False):
        for c in range(0, FF, HIDDEN):
            blocks = stack_right(rows8(adapt_b[layer, :, c:c + HIDDEN]))
            if reorder:
                moved = dot(jnp.concatenate([*blocks[:3], blocks[0]], axis=0).astype(BF16), perm[:])
                for tile in range(NT):
                    o = slice(LANES * tile, LANES * tile + LANES)
                    hi, mid, lo = moved[0:8, o], moved[8:16, o], moved[16:24, o]
                    first = UP_TILE * tile + c // HIDDEN * LANES
                    write_blocks(b6.at[:, first:first + LANES], (hi, mid, lo, hi, mid, hi))
            else:
                write_blocks(b6.at[:, c:c + HIDDEN], blocks)
        write_blocks(a6, stack_right(rows8(adapt_a[layer])))

    def normalize(layer, save):
        @pl.loop(0, TOKENS // LANES)
        def _(i):
            r = pl.ds(pl.multiple_of(i * LANES, LANES), LANES)
            xf = x[r, :].astype(F32)
            inv = lax.rsqrt(jnp.mean(xf * xf, axis=-1, keepdims=True) + NORM_EPS)
            u[r, :] = (xf * inv).astype(BF16)
            inv_s[layer, r, :] = jnp.broadcast_to(inv, (LANES, LANES))

        if layer < LAYERS - 1:
            adapters(layer)
        low = sum3(dot_t(a6[0:32, :], u[:]))
        left = stack_left(low)
        v3[layer, :, :] = jnp.concatenate([left[0], left[3], left[5]], axis=0)
        wide = jnp.concatenate(list(left) + [jnp.zeros((80, TOKENS), F32)], axis=0)
        v6[:] = jnp.transpose(wide).astype(BF16)
        if save:
            save_x(layer).start()
            save_u(layer).start()

    def save_x(layer):
        return pltpu.make_async_copy(x, resids.at[layer], load_sem.at[4])

    def save_u(layer):
        return pltpu.make_async_copy(u, normeds.at[layer], load_sem.at[5])

    def first_load(layer, t, buf):
        return pltpu.make_async_copy(land_up.at[lax.rem(layer, 2), :, pl.ds(pl.multiple_of(UP_TILE * t, LANES), UP_TILE)], buf.at[lax.rem(t, 2)], w_sem.at[0, lax.rem(t, 2)])

    def act_store(layer, t, acts):
        return pltpu.make_async_copy(acts.at[lax.rem(t, 2)], slopes.at[layer, :, pl.ds(pl.multiple_of(UP_TILE * t, LANES), UP_TILE)], act_sem.at[lax.rem(t, 2)])

    def keep_half(layer, t, h, buf):
        block = 2 * t + h - 5 * quarter
        copy = pltpu.make_async_copy(buf.at[lax.rem(t, 2), :, 256 * h:256 * h + 256],
                                     back_up.at[layer, 0, :, pl.ds(pl.multiple_of(256 * jnp.clip(block, 0, 4), LANES), 256)], keep_sem.at[h])
        return jnp.logical_and(block >= 0, block < 5), copy

    def first_product(layer, t, buf, acts, s):
        first_load(layer, t, buf).wait()
        for h in range(2):
            cond, copy = keep_half(layer, t, h, buf)
            pl.when(cond)(copy.start)

        @pl.when(t >= 2)
        def _():
            act_store(layer, t - 2, acts).wait()

        c = pl.ds(pl.multiple_of(UP_TILE * t, LANES), UP_TILE)
        pre = dot(u[:], buf[lax.rem(t, 2)]) + dot(v6[:], b6[:, c])
        act = pre.astype(BF16)
        hidden, slope = gelu_both(act)
        s[:, c] = hidden.astype(BF16)
        acts[lax.rem(t, 2)] = slope
        act_store(layer, t, acts).start()
        for h in range(2):
            cond, copy = keep_half(layer, t, h, buf)
            pl.when(cond)(copy.wait)

    def second_load(layer, c, buf):
        return pltpu.make_async_copy(land_down.at[lax.rem(layer, 2), :, pl.ds(pl.multiple_of(OUT_COLS * c, LANES), OUT_COLS)], buf.at[lax.rem(c, 2)], w_sem.at[1, lax.rem(c, 2)])

    def second_keep(layer, c, buf):
        cc = pl.ds(pl.multiple_of(OUT_COLS * c, LANES), OUT_COLS)
        return pltpu.make_async_copy(buf.at[lax.rem(c, 2), pl.ds(pl.multiple_of(QUARTER * quarter, 16), QUARTER), :], back_down.at[layer, 0, :, cc], keep_sem.at[2])

    def second_product(layer, c, buf, s):
        second_load(layer, c, buf).wait()
        keep = second_keep(layer, c, buf)
        keep.start()
        cc = pl.ds(pl.multiple_of(OUT_COLS * c, LANES), OUT_COLS)
        x[:, cc] = (x[:, cc].astype(F32) + dot(s[:], buf[lax.rem(c, 2)])).astype(BF16)
        keep.wait()

    def gelu_both(act):
        af = act.astype(F32)
        x2, th = gelu_inner(af)
        half = 0.5 * af
        slope = 0.5 + 0.5 * th + half * (1.0 - th * th) * (GELU_S + (3.0 * GELU_S * GELU_C) * x2)
        return half + half * th, slope

    def low_parts(layer, dpre, *places):
        width = dpre.shape[1] // len(places)
        dlow[:] += sum3(dot_t(jnp.concatenate([b6[0:32, pl.ds(c, width)] for c in places], axis=1), dpre))
        share = sum3(dot(v3[layer].astype(BF16), dpre))
        for i, c in enumerate(places):
            gb[:, pl.ds(c, width)] = share[:, width * i:width * i + width]

    def natural_order():
        for m in range(FF // HIDDEN):
            piece = jnp.concatenate([grad_b[LAYERS - 1, :, UP_TILE * tile + LANES * m:UP_TILE * tile + LANES * m + LANES] for tile in range(NT)], axis=1)
            parts = jnp.concatenate(split3(rows8(piece)), axis=0).astype(BF16)
            gb[:, HIDDEN * m:HIDDEN * m + HIDDEN] = sum3(dot_t(parts, perm[:]))
        grad_b[LAYERS - 1, :, :] = gb[0:RANK, :]

    def close_layer(layer, acc):
        left = stack_left(dlow[:])
        wide = jnp.concatenate(list(left) + [jnp.zeros((80, TOKENS), F32)], axis=0)
        v6[:] = jnp.transpose(wide).astype(BF16)
        narrow = jnp.concatenate([left[0], left[3], left[5]], axis=0).astype(BF16)
        ga = sum3(dot(narrow, u[:]))
        send_g[layer, 0:RANK, 0:G_EDGE] = gb[0:RANK, 0:G_EDGE]
        send_g[layer, RANK:2 * RANK, 0:FF - G_EDGE] = gb[0:RANK, G_EDGE:FF]
        send_g[layer, RANK:2 * RANK, FF - G_EDGE:G_EDGE] = ga[0:RANK]
        send_g[layer, :, G_EDGE:G_COLS] = jnp.zeros((8, G_COLS - G_EDGE), F32)
        g_step(layer, 0)

        @pl.loop(0, TOKENS // OUT_COLS)
        def _(i):
            r = pl.ds(pl.multiple_of(i * OUT_COLS, OUT_COLS), OUT_COLS)
            pl.when(jnp.logical_and(layer == 0, i == 1))(lambda: g_step(0, 1))
            side = dot(v6[r, :], a6[:]).astype(BF16)
            dn = (acc[r, :].astype(BF16) + side).astype(F32)
            xf = x[r, :].astype(F32)
            inv = inv_s[layer, r, 0:1]
            row = jnp.mean(xf * dn, axis=-1, keepdims=True)
            d[r, :] = (d[r, :].astype(F32) + inv * dn - xf * (inv * inv * inv * row)).astype(BF16)

    zero128 = jnp.zeros((80, HIDDEN), BF16)
    a6[48:LANES, :] = zero128
    for c in range(0, FF, HIDDEN):
        b6[48:LANES, c:c + HIDDEN] = zero128

    def forward(buf_a, buf_b, s, acts):
        def iteration(j, carry):
            i = j - LEAD

            pl.when(i == MIX - FAR_LEAD)(wait_credits)
            gather_step(i)

            @pl.when(i == -2)
            def _():
                loads[2].wait()
                normalize(0, True)

            second = i >= 2 * NT + 4
            layer = jnp.where(second, 1, 0)
            lo = jnp.where(second, 2 * NT + 5, 1)

            @pl.when(jnp.logical_and(i >= lo - 1, i < lo - 1 + NT))
            def _():
                first_load(layer, i - lo + 1, buf_a).start()

            @pl.when(jnp.logical_and(i >= lo, i < lo + NT))
            def _():
                first_product(layer, i - lo, buf_a, acts, s)

            @pl.when(i == lo + NT)
            def _():
                act_store(layer, NT - 2, acts).wait()
                act_store(layer, NT - 1, acts).wait()

            pl.when(i == NT + 2)(build_order)
            pl.when(i == MIX - 3)(lambda: adapters(LAYERS - 1, reorder=True))
            pieces = HIDDEN // OUT_COLS
            prev = jnp.where(i >= 4 * NT - 1, 1, 0)
            lo2 = 2 * NT + 2 * NT * prev

            @pl.when(jnp.logical_and(i >= lo2 - 1, i < lo2 - 1 + pieces))
            def _():
                second_load(prev, i - lo2 + 1, buf_b).start()

            @pl.when(i == lo2)
            def _():
                save_x(prev).wait()
                save_u(prev).wait()

            @pl.when(jnp.logical_and(i >= lo2, i < lo2 + pieces))
            def _():
                second_product(prev, i - lo2, buf_b, s)

            @pl.when(i == 2 * NT + pieces - 1)
            def _():
                give_credits()
                normalize(1, True)

            @pl.when(i == 4 * NT + pieces - 1)
            def _():
                normalize(2, False)
            return carry

        lax.fori_loop(0, FUSED_FROM + LEAD, iteration, 0)

    pl.run_scoped(
        forward,
        pltpu.VMEM((2, HIDDEN, UP_TILE), BF16), pltpu.VMEM((2, FF, OUT_COLS), BF16),
        pltpu.VMEM((TOKENS, FF), BF16), pltpu.VMEM((2, TOKENS, UP_TILE), F32),
    )

    loads[3].wait()

    last = LAYERS - 1

    def fused_loads(t, buf_a, buf_b):
        rows = land_down.reshape(2, 32, DOWN_ROWS, HIDDEN).at[last % 2, :, pl.ds(pl.multiple_of(DOWN_TILE * t, 16), DOWN_TILE), :]
        return first_load(last, t, buf_a), pltpu.make_async_copy(rows, buf_b.at[lax.rem(t, 2)], w_sem.at[1, lax.rem(t, 2)])

    def fused(buf_a, buf_b, dpre, y, acc, out):
        y[:] = jnp.zeros_like(y)
        acc[:] = jnp.zeros_like(acc)
        dlow[:] = jnp.zeros_like(dlow)
        for matrix in range(2):
            swap_own(LAYERS - 2, matrix).start()

        for load in fused_loads(0, buf_a, buf_b):
            load.start()

        def iteration(i, carry):
            gather_step(i)
            early, ticks = i - BACK_FROM, lax.rem(i - BACK_FROM, BACK_EVERY)
            pl.when(jnp.logical_and(jnp.logical_and(early >= 0, i < BACK_STEADY), ticks == 0))(lambda: send_back(early // BACK_EVERY))
            pl.when(i >= BACK_STEADY)(lambda: send_back(BACK_EARLY + i - BACK_STEADY))

            catch_up = i < FUSED_FROM + 2
            t_load = jnp.where(i == FUSED_FROM, 1, (i - MIX - 2) // 2)

            @pl.when(jnp.logical_and(jnp.logical_or(i == FUSED_FROM, lax.rem(i, 2) == 0), t_load < NT))
            def _():
                for load in fused_loads(t_load, buf_a, buf_b):
                    load.start()

            first_half = jnp.where(catch_up, 2 * (i - FUSED_FROM), i - FUSED_FROM + 2)

            @pl.loop(first_half, jnp.where(catch_up, first_half + 2, first_half + 1))
            def _(g):
                t, h = g // 2, lax.rem(g, 2)
                slot = lax.rem(t, 2)

                @pl.when(h == 0)
                def _():
                    for load in fused_loads(t, buf_a, buf_b):
                        load.wait()

                c = pl.multiple_of(UP_TILE * t, LANES)
                r = pl.ds(pl.multiple_of(ROWS * h, ROWS), ROWS)
                down = buf_b.at[slot]
                pre = dot(u[r, :], buf_a[slot]) + dot(v6[r, :], b6[:, pl.ds(c, UP_TILE)])
                dh = dot_t(d[r, :], down[:].reshape(UP_TILE, HIDDEN)).astype(BF16).astype(F32)
                s, slope = gelu_both(pre.astype(BF16))
                dp = (dh * slope).astype(BF16)
                dpre[r, :] = dp
                y[r, :] += dot(s.astype(BF16), down[:].reshape(UP_TILE, HIDDEN))
                acc[r, :] += dot_t(dp, buf_a[slot])

                @pl.when(h == 1)
                def _():
                    low_parts(last, dpre[:], c)
            return carry

        lax.fori_loop(FUSED_FROM, FUSED_TO, iteration, 0)

        pl.loop(BACK_SENT, BACK_SENT + BACK_AHEAD)(send_back)

        @pl.loop(0, TOKENS // LANES)
        def _(i):
            r = pl.ds(pl.multiple_of(i * LANES, LANES), LANES)
            out[r, :] = (x[r, :].astype(F32) + y[r, :]).astype(BF16)

        out_copy = pltpu.make_async_copy(out, out_tokens, load_sem.at[6])
        out_copy.start()
        close_layer(last, acc)
        out_copy.wait()

    pl.run_scoped(
        fused,
        pltpu.VMEM((2, HIDDEN, UP_TILE), BF16), pltpu.VMEM((2, 32, DOWN_TILE, HIDDEN), BF16), pltpu.VMEM((TOKENS, UP_TILE), BF16),
        pltpu.VMEM((TOKENS, HIDDEN), F32), pltpu.VMEM((TOKENS, HIDDEN), F32), pltpu.VMEM((TOKENS, HIDDEN), BF16),
    )

    steps = 2 * SUBS

    def backward(buf_a, buf_b, act, dpre, acc):
        def place(n):
            layer, b = (LAYERS - 2) - n // steps, lax.rem(n, steps)
            outside, sub = b // SUBS, lax.rem(b, SUBS)
            base = 2 * (parity + outside - 2 * parity * outside)
            return layer, b, outside, sub, [pl.multiple_of(QUARTER * (base + c) + SUB * sub, SUB) for c in (core, 1 - core)]

        def loads_of(n):
            layer, _, outside, sub, fs = place(n)
            s = lax.rem(n, 2)
            copies = []
            for i in range(2):
                half = pl.ds(SUB * i, SUB)
                copies += [(back_ref(0, layer, 2 * outside + i, sub), buf_a.at[s, :, half]), (back_ref(1, layer, 2 * outside + i, sub), buf_b.at[s, half, :]),
                           (slopes.at[layer, :, pl.ds(fs[i], SUB)], act.at[s, :, half])]
            return [pltpu.make_async_copy(src, dst, back_sem.at[s, i]) for i, (src, dst) in enumerate(copies)]

        def pass_on(n):
            layer, _, outside, sub, _ = place(n)

            @pl.when(jnp.logical_and(n < 2 * steps, outside == 1))
            def _():
                for matrix in range(2):
                    for axis in range(3):
                        back_copy(matrix, layer, sub, axis).wait_recv()
                    swap_sub(matrix, layer, sub).start()

        def fetch(n):
            layer, b, outside, sub, _ = place(n)

            @pl.when(b == 0)
            def _():
                for matrix in range(2):
                    swap_own(layer, matrix).wait_recv()

            @pl.when(outside == 1)
            def _():
                for matrix in range(2):
                    swap_sub(matrix, layer, sub).wait_recv()

            for load in loads_of(n):
                load.start()

        def reloads(layer):
            return (pltpu.make_async_copy(resids.at[layer], x, load_sem.at[4]), pltpu.make_async_copy(normeds.at[layer], u, load_sem.at[5]))

        for matrix in range(2):
            swap_own(0, matrix).start()
        fetch(0)

        def iteration(n, carry):
            layer, b, _, _, fs = place(n)
            s = lax.rem(n, 2)

            @pl.when(b == 0)
            def _():
                for load in reloads(layer):
                    load.start()
                adapters(layer)
                acc[:] = jnp.zeros_like(acc)
                dlow[:] = jnp.zeros_like(dlow)

            h = n + BACK_SENT + BACK_AHEAD
            pl.when(h < 4 * SUBS)(lambda: send_back(h))
            for stage in range(1, G_STAGES + 1):
                for done in range(1, LAYERS):
                    pl.when(n == SUMS_FROM + stage - done)(lambda: g_step(done, stage))
            for load in loads_of(n):
                load.wait()
            pass_on(n + 2)
            pl.when(n + 1 < 2 * steps)(lambda: fetch(n + 1))
            for h in range(TOKENS // ROWS):
                r = slice(ROWS * h, ROWS * h + ROWS)
                dh = dot_t(d[r, :], buf_b[s]).astype(BF16).astype(F32)
                dp = (dh * act[s, r, :]).astype(BF16)
                dpre[r, :] = dp
                acc[r, :] += dot_t(dp, buf_a[s])
            low_parts(layer, dpre[:], *fs)

            @pl.when(b == steps - 1)
            def _():
                for load in reloads(layer):
                    load.wait()
                close_layer(layer, acc)
            return carry

        lax.fori_loop(0, 2 * steps, iteration, 0)
        grad_copy = pltpu.make_async_copy(d, grad_tokens, load_sem.at[6])
        grad_copy.start()
        g_step(0, 2)
        pl.loop(1, LAYERS)(g_finish)
        natural_order()
        for stage in range(3, G_STAGES + 1):
            g_step(0, stage)
        g_finish(0)
        grad_copy.wait()

    pl.run_scoped(
        backward,
        pltpu.VMEM((2, HIDDEN, 2 * SUB), BF16), pltpu.VMEM((2, 2 * SUB, HIDDEN), BF16), pltpu.VMEM((2, TOKENS, 2 * SUB), F32),
        pltpu.VMEM((TOKENS, 2 * SUB), BF16), pltpu.VMEM((TOKENS, HIDDEN), F32),
    )

    @pl.loop(0, LAYERS - 1)
    def _(layer):
        for matrix in range(2):
            swap_own(layer, matrix).wait_send()

            @pl.loop(0, SUBS)
            def _(sub):
                swap_sub(matrix, layer, sub).wait_send()
                for axis in range(3):
                    back_copy(matrix, layer, sub, axis).wait_send()


def step(tokens, cotangent, w_up, w_down, adapt_a, adapt_b):
    any_spec, vmem = pl.BlockSpec(memory_space=pl.ANY), pl.BlockSpec(memory_space=pltpu.VMEM)
    sds = jax.ShapeDtypeStruct
    dma = pltpu.SemaphoreType.DMA
    outs = [
        (sds((TOKENS, HIDDEN), BF16), any_spec), (sds((TOKENS, HIDDEN), BF16), any_spec),
        (sds((LAYERS, RANK, HIDDEN), F32), vmem), (sds((LAYERS, RANK, FF), F32), vmem),
        (sds((2, HIDDEN, FF), BF16), any_spec), (sds((2, FF, HIDDEN), BF16), any_spec),
        (sds((2, 4, HIDDEN, QUARTER), BF16), any_spec), (sds((2, 4, QUARTER, HIDDEN), BF16), any_spec),
        (sds((2, TOKENS, FF), F32), any_spec), (sds((2, TOKENS, HIDDEN), BF16), any_spec), (sds((2, TOKENS, HIDDEN), BF16), any_spec),
    ]
    result = pl.pallas_call(
        step_kernel,
        out_shape=[o[0] for o in outs],
        in_specs=[any_spec] * 4 + [vmem] * 2,
        out_specs=[o[1] for o in outs],
        scratch_shapes=[
            pltpu.VMEM((LAYERS, UP_ROWS, FF), BF16), pltpu.VMEM((LAYERS, DOWN_ROWS, HIDDEN), BF16),
            pltpu.VMEM((TOKENS, HIDDEN), BF16), pltpu.VMEM((TOKENS, HIDDEN), BF16), pltpu.VMEM((TOKENS, HIDDEN), BF16),
            pltpu.VMEM((LAYERS, TOKENS, LANES), F32), pltpu.VMEM((LANES, FF), BF16), pltpu.VMEM((LANES, HIDDEN), BF16),
            pltpu.VMEM((TOKENS, LANES), BF16), pltpu.VMEM((LAYERS, 24, TOKENS), F32), pltpu.VMEM((HIDDEN, HIDDEN), BF16), pltpu.VMEM((8, TOKENS), F32), pltpu.VMEM((8, FF), F32),
            pltpu.VMEM((LAYERS, 8, G_COLS), F32), pltpu.VMEM((LAYERS, 5, 8, G_HALF), F32), pltpu.VMEM((LAYERS, 8, G_HALF), F32),
            pltpu.VMEM((LAYERS, 4, 8, G_HALF), F32), pltpu.VMEM((LAYERS, 8, G_HALF), F32),
            dma((RING, 16)), dma((RING, 4)), dma((SRING, 22)), dma((2, 2, SUBS, 3)), dma((2, 2, SUBS, 3)), dma((2, 2, SUBS + 1)), dma((2, 2, SUBS + 1)),
            dma((LAYERS, G_STAGES)), dma((LAYERS, G_STAGES)), dma((7,)), dma((2, 6)), dma((2, 2)), dma((2,)), dma((3,)), pltpu.SemaphoreType.REGULAR,
        ],
        compiler_params=pltpu.CompilerParams(collective_id=0, has_side_effects=True, vmem_limit_bytes=67_000_000),
        cost_estimate=pl.CostEstimate(flops=12 * 2 * TOKENS * HIDDEN * FF, bytes_accessed=400_000_000, transcendentals=0),
        name="mlp_stack",
    )(tokens, cotangent, w_up, w_down, jnp.swapaxes(adapt_a, 1, 2), adapt_b)
    return result[0], result[1], jnp.swapaxes(result[2], 1, 2), result[3]


def solution(mesh):
    tok_spec, weight_spec = P(GROUP, None), P(None, GROUP, None)
    return jax.shard_map(step, mesh=mesh, in_specs=(tok_spec, tok_spec, weight_spec, weight_spec, P(), P()), out_specs=(tok_spec, tok_spec, P(), P()), check_vma=False)
```
